256 devices in a mesh: seq: 64 (over x, y, z_lo), head: 4 (over z_hi, core).
Axes of the slice: x: 4, y: 4, z: 8 (z_hi: 2, z_lo: 4; z = z_hi * 4 + z_lo), core: 2. Of those that a mesh axis runs over, the one named last changes fastest.
Arguments:
- prompt_token_query: bfloat16 [2048, 8192], P('seq', 'head'), may hold values from -6 to 6
- prompt_token_key: bfloat16 [2048, 1024], P('seq', 'head'), may hold values from -6 to 6
- prompt_token_value: bfloat16 [2048, 1024], P('seq', 'head'), may hold values from -6 to 6
- response_query_slots: bfloat16 [12288, 8192], P('seq', 'head'), may hold values from -160 to 160
- response_key_slots: bfloat16 [12288, 1024], P('seq', 'head'), may hold values from -6 to 6
- response_value_slots: bfloat16 [12288, 1024], P('seq', 'head'), may hold values from -6 to 6
- lengths: int32 [16], replicated, may hold values from 1 to 32, 64 in all
- block_table: int32 [64], replicated, may hold values from 0 to 63, each once
Outputs:
- prompt_out: bfloat16 [2048, 8192], P(('seq', 'head'))
- answer_out: bfloat16 [12288, 8192], P(('seq', 'head'))
The draws below stay inside these ranges and needn't reach their ends.
Inputs may be any that keep to these rules, and one draw needn't show every extreme that they name: `lengths`: they sum to 64; the largest is exactly 32. `block_table`: A permutation of 0 to 63.
All inputs are finite; a program needn't handle non-finite values.
Results may differ from the reference program's by a relative error of at most 0.007.
Values may be sent and summed in bfloat16 or wider, within the bound.
No kernel may reach another device: no remote copies, remote signals or barrier semaphores. Data moves between devices by JAX's collectives and lax.ppermute only.
A program may use at most 64 MiB of HBM per device.

```python
import math
import jax
import jax.numpy as jnp
import numpy as np
from jax import lax

QUERY_HEADS = 64
KEY_VALUE_HEADS = 8
HEAD_SIZE = 128
RESPONSE_BLOCK = 192
PROMPT_PER_SEQ = 32
MEMBERS = 16
RESPONSE_COUNT = 64
LONGEST_BLOCKS = 32
PROMPT_TOKENS = 2048
RESPONSE_TOKENS = 12288
N_SEQ = 64


def paired_keys(key):
    regular_portion = jnp.clip(jax.random.normal(jax.random.fold_in(key, 7001), (PROMPT_TOKENS, KEY_VALUE_HEADS, HEAD_SIZE), jnp.float32), -6.0, 6.0)
    return regular_portion


def draw_prompt_token_key(key, part):
    key_lookup_table = paired_keys(key)
    return key_lookup_table.reshape(PROMPT_TOKENS, KEY_VALUE_HEADS * HEAD_SIZE).astype(jnp.bfloat16)


def draw_response_query_slots(key, part):
    regular_portion = jnp.clip(jax.random.normal(jax.random.fold_in(key, 7003), (RESPONSE_TOKENS, QUERY_HEADS, HEAD_SIZE), jnp.float32), -6.0, 6.0)
    return regular_portion.reshape(RESPONSE_TOKENS, QUERY_HEADS * HEAD_SIZE).astype(jnp.bfloat16)


def shard_levels(key, shape, shards, smallest, high):
    def one(dim, parts):
        steps = jax.random.uniform(jax.random.fold_in(jax.random.fold_in(key, 6), dim), (parts,), jnp.float32, smallest / len(shards), high / len(shards))
        return jnp.repeat(jnp.exp(steps), shape[dim] // parts).reshape((-1,) + (1,) * (len(shape) - dim - 1))

    loudness = one(*shards[0])
    for cut in shards[1:]:
        loudness = loudness * one(*cut)
    return loudness


def length_profile(count, total, most, skew):
    portions = [(1 << 20) // math.isqrt(grade ** skew) + 1 for grade in range(2, count + 1)]
    surplus, given = total - most - (count - 1), [1] * (count - 1)
    while surplus > 0:
        candidates = [i for i in range(count - 1) if given[i] < most]
        whole, budget = sum([portions[i] for i in candidates]), surplus
        for i in candidates:
            extra = min(most - given[i], max(1, budget * portions[i] // whole), surplus)
            given[i] = given[i] + extra
            surplus = surplus - extra
    return np.array([most] + given)


def ragged_sizes(stream_key, amount, total, most, slope):
    if amount == 2:
        one = jax.random.randint(stream_key, (), max(1, total - most), min(most, total - 1) + 1)
        return jnp.stack([one, total - one])
    tallies = jnp.asarray(length_profile(amount, total, most, slope), jnp.int32)
    twos = (amount - 1) // 2
    donor, sink = tallies[1:1 + 2 * twos:2], tallies[2:2 + 2 * twos:2]
    margin = jnp.minimum(donor - 1, most - sink)
    shifted = jax.random.randint(jax.random.fold_in(stream_key, 1), (twos,), 0, 1 << 20) % (margin + 1)
    tallies = tallies.at[1:1 + 2 * twos:2].set(donor - shifted).at[2:2 + 2 * twos:2].set(sink + shifted)
    return tallies[jax.random.permutation(jax.random.fold_in(stream_key, 2), amount)]


def gaussian(rng, shape, deviation, limit, cuts=(), held_as=jnp.bfloat16):
    values = jax.random.normal(rng, shape, jnp.float32) * deviation
    if len(cuts) > 0:
        values = shard_levels(rng, shape, cuts, -0.22, 0.18) * values
    return jnp.clip(values, min=-limit, max=limit).astype(held_as)


def setup_inputs(seed: int = 0) -> dict:
    streams_of = jax.random.split(jax.random.key(seed), 9)
    return {
        "prompt_token_query": gaussian(streams_of[0], (PROMPT_TOKENS, QUERY_HEADS * HEAD_SIZE), 1.0, 6.0, ((0, 64), (1, 4))),
        "prompt_token_key": draw_prompt_token_key(jax.random.fold_in(streams_of[8], 71), 0),
        "prompt_token_value": gaussian(streams_of[2], (PROMPT_TOKENS, KEY_VALUE_HEADS * HEAD_SIZE), 1.0, 6.0, ((0, 64), (1, 4))),
        "response_query_slots": draw_response_query_slots(jax.random.fold_in(streams_of[8], 71), 0),
        "response_key_slots": gaussian(streams_of[4], (RESPONSE_TOKENS, KEY_VALUE_HEADS * HEAD_SIZE), 1.0, 6.0, ((0, 64), (1, 4))),
        "response_value_slots": gaussian(streams_of[5], (RESPONSE_TOKENS, KEY_VALUE_HEADS * HEAD_SIZE), 1.0, 6.0, ((0, 64), (1, 4))),
        "lengths": ragged_sizes(streams_of[6], MEMBERS, RESPONSE_COUNT, LONGEST_BLOCKS, 2).astype(jnp.int32),
        "block_table": jax.random.permutation(streams_of[7], RESPONSE_COUNT).astype(jnp.int32),
    }


def block_roles(lengths, global_blocks):
    bounds = jnp.cumsum(lengths).astype(jnp.int32)
    member = jnp.sum((global_blocks[:, None] >= bounds[None, :]).astype(jnp.int32), axis=1).astype(jnp.int32)
    starts = (bounds - lengths).astype(jnp.int32)
    owner_match = member[:, None] == jnp.arange(lengths.shape[0], dtype=jnp.int32)[None, :]
    first_block = jnp.sum(jnp.where(owner_match, starts[None, :], 0), axis=1).astype(jnp.int32)
    return member, (global_blocks - first_block).astype(jnp.int32), first_block


def attend(query_matrix, key_rows, value_rows, visible):
    scores = jnp.einsum("rjgd,sjd->rjgs", query_matrix.astype(jnp.float32), key_rows.astype(jnp.float32)) * (HEAD_SIZE ** -0.5)
    seen = visible[:, None, None, :]
    masked = jnp.where(seen, scores, -jnp.inf)
    peak_value = jnp.max(masked, axis=-1, keepdims=True)
    weights = jnp.where(seen, jnp.exp(scores - peak_value), 0.0)
    weight_total = jnp.sum(weights, axis=-1)
    rounded = weights.astype(jnp.bfloat16).astype(jnp.float32)
    mixed_sum = jnp.einsum("rjgs,sjd->rjgd", rounded, value_rows.astype(jnp.float32))
    return (mixed_sum / weight_total[..., None]).astype(jnp.bfloat16)


def reference(prompt_token_query, prompt_token_key, prompt_token_value, response_query_slots, response_key_slots, response_value_slots, lengths, block_table):
    query_group_width = QUERY_HEADS // KEY_VALUE_HEADS
    shared_prompt_keys = prompt_token_key.reshape(PROMPT_TOKENS, KEY_VALUE_HEADS, HEAD_SIZE)
    shared_prompt_values = prompt_token_value.reshape(PROMPT_TOKENS, KEY_VALUE_HEADS, HEAD_SIZE)

    def prompt_block(leading_row):
        query_matrix = lax.dynamic_slice_in_dim(prompt_token_query, leading_row, PROMPT_PER_SEQ, 0).reshape(PROMPT_PER_SEQ, KEY_VALUE_HEADS, query_group_width, HEAD_SIZE)
        query_positions = leading_row + jnp.arange(PROMPT_PER_SEQ, dtype=jnp.int32)
        visible = jnp.arange(PROMPT_TOKENS, dtype=jnp.int32)[None, :] <= query_positions[:, None]
        return attend(query_matrix, shared_prompt_keys, shared_prompt_values, visible).reshape(PROMPT_PER_SEQ, QUERY_HEADS * HEAD_SIZE)

    prompt_out = lax.map(prompt_block, jnp.arange(N_SEQ, dtype=jnp.int32) * PROMPT_PER_SEQ).reshape(PROMPT_TOKENS, QUERY_HEADS * HEAD_SIZE)

    inverse = jnp.argsort(block_table).astype(jnp.int32)
    blocked_keys = response_key_slots.reshape(RESPONSE_COUNT, RESPONSE_BLOCK, KEY_VALUE_HEADS, HEAD_SIZE)
    blocked_values = response_value_slots.reshape(RESPONSE_COUNT, RESPONSE_BLOCK, KEY_VALUE_HEADS, HEAD_SIZE)
    member, position, first_block = block_roles(lengths, block_table)

    def answer_block(slot_ordinal):
        query_matrix = lax.dynamic_slice_in_dim(response_query_slots, slot_ordinal * RESPONSE_BLOCK, RESPONSE_BLOCK, 0).reshape(RESPONSE_BLOCK, KEY_VALUE_HEADS, query_group_width, HEAD_SIZE)
        own_position = position[slot_ordinal]
        span = jnp.minimum(first_block[slot_ordinal] + jnp.arange(LONGEST_BLOCKS, dtype=jnp.int32), RESPONSE_COUNT - 1)
        window_slots = inverse[span]
        window_keys = blocked_keys[window_slots].reshape(LONGEST_BLOCKS * RESPONSE_BLOCK, KEY_VALUE_HEADS, HEAD_SIZE)
        window_values = blocked_values[window_slots].reshape(LONGEST_BLOCKS * RESPONSE_BLOCK, KEY_VALUE_HEADS, HEAD_SIZE)
        key_positions = jnp.arange(LONGEST_BLOCKS * RESPONSE_BLOCK, dtype=jnp.int32)
        query_positions = own_position * RESPONSE_BLOCK + jnp.arange(RESPONSE_BLOCK, dtype=jnp.int32)
        own_visible = key_positions[None, :] <= query_positions[:, None]
        visible = jnp.concatenate([jnp.ones((RESPONSE_BLOCK, PROMPT_TOKENS), dtype=bool), own_visible], axis=1)
        all_keys = jnp.concatenate([shared_prompt_keys, window_keys], axis=0)
        all_values = jnp.concatenate([shared_prompt_values, window_values], axis=0)
        return attend(query_matrix, all_keys, all_values, visible).reshape(RESPONSE_BLOCK, QUERY_HEADS * HEAD_SIZE)

    answer_out = lax.map(answer_block, jnp.arange(RESPONSE_COUNT, dtype=jnp.int32)).reshape(RESPONSE_TOKENS, QUERY_HEADS * HEAD_SIZE)
    return prompt_out, answer_out
```

```python
import functools

import jax
import jax.numpy as jnp
from jax import lax
from jax.experimental import pallas as pl
from jax.experimental.pallas import tpu as pltpu
from jax.sharding import Mesh, PartitionSpec as P

D = 128
RB = 192
PR = 32
LOG_SCALE = (128 ** -0.5) * 1.4426950408889634
NEG = -1e30


def roles(seq, len_ref, tab_ref, order_ref, members, slots):
    own = tab_ref[seq]
    def find(m, c):
        start, first = c
        n = len_ref[m]
        hit = (own >= start) & (own < start + n)
        return start + n, jnp.where(hit, start, first)
    _, first = lax.fori_loop(0, members, find, (jnp.int32(0), jnp.int32(0)))
    def place(s, c):
        g = tab_ref[s]
        @pl.when((g >= first) & (g <= own))
        def _():
            order_ref[g - first] = s
        return c
    lax.fori_loop(0, slots, place, jnp.int32(0))
    return own - first + 1


def step(q, k, v, m_ref, l_ref, a_ref, idx, mask):
    t = lax.dot_general(q, k, (((1,), (1,)), ((), ())), preferred_element_type=jnp.float32) * LOG_SCALE
    if mask is not None:
        t = jnp.where(mask, t, NEG)
    m_old = m_ref[idx]
    m_new = jnp.maximum(m_old, jnp.max(t, axis=1, keepdims=True))
    alpha = jnp.exp2(m_old - m_new)
    p = jnp.exp2(t - m_new[:, :1])
    m_ref[idx] = m_new
    l_ref[idx] = l_ref[idx] * alpha + jnp.sum(p, axis=1, keepdims=True)
    a_ref[idx] = a_ref[idx] * alpha + lax.dot_general(
        p.astype(jnp.bfloat16), v, (((1,), (0,)), ((), ())), preferred_element_type=jnp.float32)


def kernel(seq_ref, len_ref, tab_ref, pq_ref, rq_ref, kv_ref, out_ref,
           order_ref, pkv, rkv, qs, pqs, m, l, a, pm, plr, pa, psem, rsem, *, PC, RC, slots, members):
    seq = seq_ref[0]
    nh = rq_ref.shape[1] // D
    g = 8
    pcopy = pltpu.make_async_copy(kv_ref.at[:, pl.ds(0, PR)], pkv, psem)
    pcopy.start()
    n = roles(seq, len_ref, tab_ref, order_ref, members, slots)
    def rcopy(i):
        return pltpu.make_async_copy(kv_ref.at[order_ref[i], pl.ds(PR, RB)], rkv.at[pl.ds(i * RB, RB)], rsem.at[i])
    lax.fori_loop(0, n, lambda i, c: (rcopy(i).start(), c)[1], 0)
    blocks = RC // RB
    nch = (n + blocks - 1) // blocks
    def zero(i, c):
        rkv[pl.ds(pl.multiple_of(i * RB, RB), RB), :] = jnp.zeros((RB, rkv.shape[1]), rkv.dtype)
        return c
    lax.fori_loop(n, nch * blocks, zero, 0)
    for h in range(nh):
        qs[h] = rq_ref[:, h * D:(h + 1) * D]
        pqs[h // g, (h % g) * PR:(h % g + 1) * PR] = pq_ref[:, h * D:(h + 1) * D]
    for r in (m, pm):
        r[...] = jnp.full(r.shape, NEG, jnp.float32)
    for r in (l, a, plr, pa):
        r[...] = jnp.zeros(r.shape, jnp.float32)
    pcopy.wait()
    pflat = pkv.reshape(slots * PR, pkv.shape[2])
    nk = rkv.shape[1] // 2
    def prompt_chunk(c, carry):
        rows = pl.ds(pl.multiple_of(c * PC, PC), PC)
        for j in range(nh // g):
            k = pflat[rows, j * D:(j + 1) * D]
            v = pflat[rows, nk + j * D:nk + (j + 1) * D]
            def head(h, _):
                step(qs[h], k, v, m, l, a, h, None)
                return _
            lax.fori_loop(j * g, (j + 1) * g, head, 0)
            @pl.when(c * PC <= seq * PR + PR - 1)
            def own_rows():
                key = lax.broadcasted_iota(jnp.int32, (g * PR, PC), 1) + c * PC
                row = (lax.broadcasted_iota(jnp.int32, (g * PR, PC), 0) & (PR - 1)) + seq * PR
                step(pqs[j], k, v, pm, plr, pa, j, key <= row)
        return carry
    lax.fori_loop(0, slots * PR // PC, prompt_chunk, 0)

    def resp_chunk(c, masked):
        lax.fori_loop(c * blocks, jnp.minimum(c * blocks + blocks, n), lambda i, x: (rcopy(i).wait(), x)[1], 0)
        rows = pl.ds(pl.multiple_of(c * RC, RC), RC)
        if masked:
            key = lax.broadcasted_iota(jnp.int32, (RB, RC), 1) + c * RC
            row = lax.broadcasted_iota(jnp.int32, (RB, RC), 0) + (n - 1) * RB
            mask = key <= row
        else:
            mask = None
        for j in range(nh // g):
            k = rkv[rows, j * D:(j + 1) * D]
            v = rkv[rows, nk + j * D:nk + (j + 1) * D]
            def head(h, _):
                step(qs[h], k, v, m, l, a, h, mask)
                return _
            lax.fori_loop(j * g, (j + 1) * g, head, 0)
    lax.fori_loop(0, nch - 1, lambda c, x: (resp_chunk(c, False), x)[1], 0)
    resp_chunk(nch - 1, True)
    parts = out_ref.shape[0]
    pn, rn = PR // parts, RB // parts
    for h in range(nh):
        cols = slice(h * D, (h + 1) * D)
        rr = slice((h % g) * PR, (h % g + 1) * PR)
        answer = (a[h] / l[h]).astype(jnp.bfloat16)
        prompt = (pa[h // g, rr] / plr[h // g, rr]).astype(jnp.bfloat16)
        for d in range(parts):
            out_ref[d, :pn, cols] = prompt[d * pn:(d + 1) * pn]
            out_ref[d, pn:, cols] = answer[d * rn:(d + 1) * rn]


def attention(seq, lengths, table, pq, rq, kv, parts, PC=1024, RC=768):
    slots = table.shape[0]
    nh = rq.shape[1] // D
    kvh = kv.shape[2] // (2 * D)
    longest = slots // 2
    f32 = jnp.float32
    smem = pl.BlockSpec(memory_space=pltpu.SMEM)
    vmem = pl.BlockSpec(memory_space=pltpu.VMEM)
    return pl.pallas_call(
        functools.partial(kernel, PC=PC, RC=RC, slots=slots, members=lengths.shape[0]),
        out_shape=jax.ShapeDtypeStruct((parts, (PR + RB) // parts, rq.shape[1]), jnp.bfloat16),
        in_specs=[smem, smem, smem, vmem, vmem, pl.BlockSpec(memory_space=pl.ANY)],
        out_specs=vmem,
        scratch_shapes=[
            pltpu.SMEM((longest,), jnp.int32),
            pltpu.VMEM((slots, PR, kv.shape[2]), jnp.bfloat16),
            pltpu.VMEM((longest * RB, kv.shape[2]), jnp.bfloat16),
            pltpu.VMEM((nh, RB, D), jnp.bfloat16),
            pltpu.VMEM((kvh, nh // kvh * PR, D), jnp.bfloat16),
            pltpu.VMEM((nh, RB, D), f32), pltpu.VMEM((nh, RB, D), f32), pltpu.VMEM((nh, RB, D), f32),
            pltpu.VMEM((kvh, nh // kvh * PR, D), f32), pltpu.VMEM((kvh, nh // kvh * PR, D), f32), pltpu.VMEM((kvh, nh // kvh * PR, D), f32),
            pltpu.SemaphoreType.DMA, pltpu.SemaphoreType.DMA((longest,)),
        ],
        compiler_params=pltpu.CompilerParams(vmem_limit_bytes=56 * 2**20),
        name="attention",
    )(seq, lengths, table, pq, rq, kv)


SEQ = ("x", "y", "zl")
HEAD = ("zh", "core")


def on_device(pq, pk, pv, rq, rk, rv, lengths, table):
    seq = lax.axis_index(SEQ).astype(jnp.int32).reshape(1)
    own = jnp.concatenate([jnp.concatenate([pk, pv], axis=1), jnp.concatenate([rk, rv], axis=1)], axis=0)
    line = lax.all_gather(own, "zl", axis=0, tiled=True)
    every = lax.all_gather(line, ("x", "y"), axis=0, tiled=True)
    kv = every.reshape(table.shape[0], PR + RB, own.shape[1])
    parts = lax.axis_size(HEAD)
    mixed = attention(seq, lengths, table, pq, rq, kv, parts)
    got = lax.all_to_all(mixed, HEAD, split_axis=0, concat_axis=0, tiled=True)
    pn = PR // parts
    flat = lambda t: t.transpose(1, 0, 2).reshape(t.shape[1], -1)
    return flat(got[:, :pn]), flat(got[:, pn:])


def solution(mesh):
    grid = Mesh(mesh.devices.reshape(4, 4, 4, 2, 2), SEQ + HEAD)
    both = P(SEQ, HEAD)
    rows = P(SEQ + HEAD, None)
    return jax.shard_map(
        on_device, mesh=grid, in_specs=(both,) * 6 + (P(), P()), out_specs=(rows, rows), check_vma=False
    )
```

```python
import functools

import jax
import jax.numpy as jnp
from jax import lax
from jax.experimental import pallas as pl
from jax.experimental.pallas import tpu as pltpu
from jax.sharding import Mesh, PartitionSpec as P

D = 128
RB = 192
PR = 32
G = 8
PER_EXP = 128 ** -0.5
NEG = -1e30
CH = 1024


def kernel(place_ref, len_ref, tab_ref, own_ref, got_ref, kv_ref, out_ref,
           order, kv, qs, pqs, m, l, a, pm, plr, pa, s0, s1, p0, p1, f0, f1, psem, rsem,
           *, slots, members, longest):
    pair = place_ref[0]
    side = place_ref[1]
    span = longest * RB
    base = slots * PR
    copies = [pltpu.make_async_copy(kv_ref.at[:, pl.ds(0, PR), pl.ds(w * D, D)], kv.at[w, pl.ds(0, base)].reshape(slots, PR, D), psem.at[w])
              for w in range(2)]
    for c in copies:
        c.start()

    def find(t):
        seq = 2 * pair + t
        own = tab_ref[seq]
        def look(i, c):
            start, first = c
            n = len_ref[i]
            return start + n, jnp.where((own >= start) & (own < start + n), start, first)
        _, first = lax.fori_loop(0, members, look, (jnp.int32(0), jnp.int32(0)))
        def put(s, c):
            g = tab_ref[s]
            @pl.when((g >= first) & (g <= own))
            def keep():
                order[t * longest + g - first] = s
            return c
        lax.fori_loop(0, slots, put, jnp.int32(0))
        return own - first + 1

    def fetch(t, i, w):
        return pltpu.make_async_copy(
            kv_ref.at[order[t * longest + i], pl.ds(PR, RB), pl.ds(w * D, D)],
            kv.at[w, pl.ds(base + t * span + i * RB, RB)], rsem.at[t * longest + i, w])

    counts = [find(0), find(1)]
    for t in range(2):
        def go(i, c, t=t):
            fetch(t, i, 0).start()
            fetch(t, i, 1).start()
            return c
        lax.fori_loop(0, counts[t], go, 0)
        n = counts[t]
        stop = (n * RB + CH - 1) // CH * CH
        def clear(i, c, t=t):
            kv[1, pl.ds(pl.multiple_of(base + t * span + i * 64, 64), 64), :] = jnp.zeros((64, D), jnp.bfloat16)
            return c
        lax.fori_loop(n * RB // 64, stop // 64, clear, 0)

    for src, t in ((own_ref, side), (got_ref, 1 - side)):
        for h in range(G):
            cols = slice(h * D, (h + 1) * D)
            qs[t * G + h] = src[PR:, cols]
            pqs[t, h * PR:(h + 1) * PR] = src[:PR, cols]
    for r in (m, pm):
        r[...] = jnp.full(r.shape, NEG, jnp.float32)
    for r in (l, a, plr, pa):
        r[...] = jnp.zeros(r.shape, jnp.float32)
    for c in copies:
        c.wait()

    def wide(x):
        return jnp.concatenate([x] * (CH // D), axis=1)

    def lanes(x):
        tot = x[:, :D]
        for i in range(1, CH // D):
            tot = tot + x[:, i * D:(i + 1) * D]
        return tot

    def soft(s, m_ref, l_ref, i):
        old = m_ref[i]
        new = jnp.maximum(old, jnp.max(s, axis=1, keepdims=True))
        factor = jnp.exp((old - new) * PER_EXP)
        p = jnp.exp((s - wide(new)) * PER_EXP)
        m_ref[i] = new
        l_ref[i] = l_ref[i] * factor + lanes(p)
        return p.astype(jnp.bfloat16), factor

    def scores(q, start):
        return lax.dot_general(q, kv[0, pl.ds(start, CH), :], (((1,), (1,)), ((), ())), preferred_element_type=jnp.float32)

    def mixed(p, start):
        return lax.dot_general(p, kv[1, pl.ds(start, CH), :], (((1,), (0,)), ((), ())), preferred_element_type=jnp.float32)

    for c in range(base // CH):
        for t in range(2):
            @pl.when(c * CH <= (2 * pair + t) * PR + PR - 1)
            def prompt_rows(c=c, t=t):
                key = lax.broadcasted_iota(jnp.int32, (G * PR, CH), 1) + c * CH
                row = (lax.broadcasted_iota(jnp.int32, (G * PR, CH), 0) & (PR - 1)) + (2 * pair + t) * PR
                s = jnp.where(key <= row, scores(pqs[t], c * CH), NEG)
                p, factor = soft(s, pm, plr, t)
                pa[t] = pa[t] * factor + mixed(p, c * CH)

    def answer(t, carry):
        n = jnp.where(t == 0, counts[0], counts[1])
        def where_is(u):
            c = u >> 3
            return pl.multiple_of(jnp.where(c < base // CH, c * CH, c * CH + t * span), CH)
        def stage_a(u, s):
            s[...] = scores(qs[t * G + (u & 7)], where_is(u))
        def stage_b(u, s, p, f, masked):
            x = s[...]
            if masked:
                key = lax.broadcasted_iota(jnp.int32, (RB, CH), 1) + ((u >> 3) * CH - base)
                row = lax.broadcasted_iota(jnp.int32, (RB, CH), 0) + (n - 1) * RB
                x = jnp.where(key <= row, x, NEG)
            p[...], f[...] = soft(x, m, l, t * G + (u & 7))
        def stage_c(u, p, f):
            i = t * G + (u & 7)
            a[i] = a[i] * f[...] + mixed(p[...], where_is(u))
        def run(lo, hi, masked):
            stage_a(lo, s0)
            p1[...] = jnp.zeros(p1.shape, p1.dtype)
            f1[...] = jnp.ones(f1.shape, f1.dtype)
            def two(i, c):
                u = lo + 2 * i
                stage_a(u + 1, s1)
                stage_b(u, s0, p0, f0, masked)
                stage_c(jnp.maximum(u - 1, lo), p1, f1)
                stage_a(jnp.minimum(u + 2, hi - 1), s0)
                stage_b(u + 1, s1, p1, f1, masked)
                stage_c(u, p0, f0)
                return c
            lax.fori_loop(0, (hi - lo) // 2, two, 0)
            stage_c(hi - 1, p1, f1)
        plain = base // CH + (n - 1) * RB // CH
        every = base // CH + (n * RB + CH - 1) // CH
        def landed(i, c):
            fetch(t, i, 0).wait()
            fetch(t, i, 1).wait()
            return c
        lax.fori_loop(0, n, landed, 0)
        run(0, plain * G, False)
        run(plain * G, every * G, True)
        return carry
    lax.fori_loop(0, 2, answer, 0)

    parts = out_ref.shape[0] // 2
    pn, rn = PR // parts, RB // parts
    for t in range(2):
        for h in range(G):
            cols = slice(h * D, (h + 1) * D)
            i = t * G + h
            done = (a[i] / jnp.sum(l[i], axis=1, keepdims=True)).astype(jnp.bfloat16)
            rr = slice(h * PR, (h + 1) * PR)
            asked = (pa[t, rr] / jnp.sum(plr[t, rr], axis=1, keepdims=True)).astype(jnp.bfloat16)
            for d in range(parts):
                out_ref[2 * d + t, :pn, cols] = asked[d * pn:(d + 1) * pn]
                out_ref[2 * d + t, pn:, cols] = done[d * rn:(d + 1) * rn]


def attention(place, lengths, table, own, got, kv, parts):
    slots = table.shape[0]
    longest = slots // 2
    f32, bf16 = jnp.float32, jnp.bfloat16
    smem = pl.BlockSpec(memory_space=pltpu.SMEM)
    vmem = pl.BlockSpec(memory_space=pltpu.VMEM)
    return pl.pallas_call(
        functools.partial(kernel, slots=slots, members=lengths.shape[0], longest=longest),
        out_shape=jax.ShapeDtypeStruct((2 * parts, (PR + RB) // parts, own.shape[1]), bf16),
        in_specs=[smem, smem, smem, vmem, vmem, pl.BlockSpec(memory_space=pl.ANY)],
        out_specs=vmem,
        scratch_shapes=[
            pltpu.SMEM((2 * longest,), jnp.int32),
            pltpu.VMEM((2, slots * PR + 2 * longest * RB, D), bf16),
            pltpu.VMEM((2 * G, RB, D), bf16),
            pltpu.VMEM((2, G * PR, D), bf16),
            pltpu.VMEM((2 * G, RB, D), f32), pltpu.VMEM((2 * G, RB, D), f32), pltpu.VMEM((2 * G, RB, D), f32),
            pltpu.VMEM((2, G * PR, D), f32), pltpu.VMEM((2, G * PR, D), f32), pltpu.VMEM((2, G * PR, D), f32),
            pltpu.VMEM((RB, CH), f32), pltpu.VMEM((RB, CH), f32),
            pltpu.VMEM((RB, CH), bf16), pltpu.VMEM((RB, CH), bf16),
            pltpu.VMEM((RB, D), f32), pltpu.VMEM((RB, D), f32),
            pltpu.SemaphoreType.DMA((2,)), pltpu.SemaphoreType.DMA((2 * longest, 2)),
        ],
        compiler_params=pltpu.CompilerParams(vmem_limit_bytes=56 * 2**20),
        name="attention",
    )(place, lengths, table, own, got, kv)


SEQ = ("x", "y", "zp", "zq")
HEAD = ("zh", "core")


def on_device(pq, pk, pv, rq, rk, rv, lengths, table):
    side = lax.axis_index("zq").astype(jnp.int32)
    pair = lax.axis_index(("x", "y", "zp")).astype(jnp.int32)
    half = rq.shape[1] // 2
    queries = jnp.concatenate([pq, rq], axis=0)
    give = lax.dynamic_slice_in_dim(queries, (1 - side) * half, half, 1)
    keep = lax.dynamic_slice_in_dim(queries, side * half, half, 1)
    keyval = jnp.concatenate(
        [jnp.concatenate([p[:, j * D:(j + 1) * D], r[:, j * D:(j + 1) * D]], axis=0)
         for j in range(2) for p, r in ((pk, rk), (pv, rv))], axis=1)
    line = lax.all_gather(keyval, ("zp", "zq"), axis=0, tiled=True)
    mine = lax.dynamic_slice_in_dim(line, side * 2 * D, 2 * D, 1)
    every = lax.all_gather(mine, ("x", "y"), axis=0, tiled=True)
    got = lax.ppermute(give, "zq", [(0, 1), (1, 0)])
    kv = every.reshape(table.shape[0], PR + RB, 2 * D)
    parts = lax.axis_size(HEAD)
    mixed = attention(jnp.stack([pair, side]), lengths, table, keep, got, kv, parts)
    back = lax.all_to_all(mixed, HEAD + ("zq",), split_axis=0, concat_axis=0, tiled=True)
    pn = PR // parts
    flat = lambda t: t.transpose(1, 0, 2).reshape(t.shape[1], -1)
    return flat(back[:, :pn]), flat(back[:, pn:])


def solution(mesh):
    grid = Mesh(mesh.devices.reshape(4, 4, 2, 2, 2, 2), SEQ + HEAD)
    both = P(SEQ, HEAD)
    rows = P(SEQ + HEAD, None)
    return jax.shard_map(
        on_device, mesh=grid, in_specs=(both,) * 6 + (P(), P()), out_specs=(rows, rows), check_vma=False
    )
```

```python
import functools

import jax
import jax.numpy as jnp
from jax import lax
from jax.experimental import pallas as pl
from jax.experimental.pallas import tpu as pltpu
from jax.sharding import Mesh, PartitionSpec as P

D = 128
RB = 192
PR = 32
G = 8
PER_EXP = 128 ** -0.5 * 1.4426950408889634
NEG = -1e30
CH = 1024


def kernel(place_ref, len_ref, tab_ref, own_ref, got_ref, *refs, slots, members, longest):
    pieces, (out_ref, order, kv, qs, pqs, m, a, pm, pa, s0, s1, p0, p1, f0, f1, psem, rsem) = refs[:10], refs[10:]
    px, py, pp, side = [place_ref[i] for i in range(4)]
    pair = (px * 4 + py) * 2 + pp
    span = longest * RB
    base = slots * PR
    width = 2 * D

    homes = [(c, *h) for c in range(2) for h in ((0, 0), (3, 0), (1, 0), (2, 0), (2, 2))]
    for piece, (colour, far, first) in zip(pieces, homes):
        def bring(i, c, piece=piece, colour=colour, far=far, first=first):
            near, e = i >> 1, i & 1
            dx, dy = (first + near, far) if colour == 0 else (far, first + near)
            slot = ((((px + dx) & 3) * 4 + ((py + dy) & 3)) * 2 + (pp ^ colour)) * 2 + (side ^ e)
            pltpu.make_async_copy(piece.at[near, e, pl.ds(0, PR)], kv.at[pl.ds(slot * PR, PR), pl.ds(0, width)], psem).start()
            return c
        lax.fori_loop(0, 2 * piece.shape[0], bring, 0)
    def find(t):
        seq = 2 * pair + t
        own = tab_ref[seq]
        def look(i, c):
            start, first = c
            n = len_ref[i]
            return start + n, jnp.where((own >= start) & (own < start + n), start, first)
        _, first = lax.fori_loop(0, members, look, (jnp.int32(0), jnp.int32(0)))
        def put(s, c):
            g = tab_ref[s]
            @pl.when((g >= first) & (g <= own))
            def keep():
                order[t * longest + g - first] = s
            return c
        lax.fori_loop(0, slots, put, jnp.int32(0))
        return own - first + 1

    def spot(t, i):
        return kv.at[pl.ds(base + t * span + i * RB, RB), pl.ds(0, width)], rsem.at[t * longest + i]

    def fetch(t, i):
        s = order[t * longest + i]
        e = (s & 1) ^ side
        colour = ((s >> 1) & 1) ^ pp
        dx, dy = ((s >> 4) - px) & 3, (((s >> 2) & 3) - py) & 3
        far, near = jnp.where(colour == 0, dy, dx), jnp.where(colour == 0, dx, dy)
        for piece, (c, f, first) in zip(pieces, homes):
            n = piece.shape[0]
            @pl.when((colour == c) & (far == f) & (near >= first) & (near < first + n))
            def take(piece=piece, first=first):
                dst, sem = spot(t, i)
                pltpu.make_async_copy(piece.at[near - first, e, pl.ds(PR, RB)], dst, sem).start()

    def landed(t, i):
        dst, sem = spot(t, i)
        pltpu.make_async_copy(dst, dst, sem).wait()

    counts = [find(0), find(1)]
    for t in range(2):
        def go(i, c, t=t):
            fetch(t, i)
            return c
        lax.fori_loop(0, counts[t], go, 0)
        n = counts[t]
        stop = (n * RB + CH - 1) // CH * CH
        def clear(i, c, t=t):
            kv[pl.ds(pl.multiple_of(base + t * span + i * 64, 64), 64), D:width] = jnp.zeros((64, D), jnp.bfloat16)
            return c
        lax.fori_loop(n * RB // 64, stop // 64, clear, 0)

    for src, t in ((own_ref, side), (got_ref, 1 - side)):
        for h in range(G):
            cols = slice(h * D, (h + 1) * D)
            qs[t * G + h] = src[PR:, cols]
            pqs[t, h * PR:(h + 1) * PR] = src[:PR, cols]
    for r in (m, pm):
        r[...] = jnp.full(r.shape, NEG, jnp.float32)
    for r in (a, pa):
        r[...] = jnp.zeros(r.shape, jnp.float32)
    kv[:, width:] = jnp.ones((kv.shape[0], D), jnp.bfloat16)
    pltpu.make_async_copy(kv.at[pl.ds(0, base), pl.ds(0, width)], kv.at[pl.ds(0, base), pl.ds(0, width)], psem).wait()

    def wide(x):
        return jnp.concatenate([x] * (CH // D), axis=1)

    def soft(s, m_ref, i):
        old = m_ref[i]
        new = jnp.maximum(old, jnp.max(s, axis=1, keepdims=True))
        m_ref[i] = new
        return jnp.exp2((s - wide(new)) * PER_EXP).astype(jnp.bfloat16), jnp.exp2((old - new) * PER_EXP)

    def scores(q, start):
        return lax.dot_general(q, kv[pl.ds(start, CH), :D], (((1,), (1,)), ((), ())), preferred_element_type=jnp.float32)

    def mixed(p, start):
        return lax.dot_general(p, kv[pl.ds(start, CH), D:], (((1,), (0,)), ((), ())), preferred_element_type=jnp.float32)

    def both(f):
        return jnp.concatenate([f, f], axis=1)

    for c in range(base // CH):
        for t in range(2):
            @pl.when(c * CH <= (2 * pair + t) * PR + PR - 1)
            def prompt_rows(c=c, t=t):
                key = lax.broadcasted_iota(jnp.int32, (G * PR, CH), 1) + c * CH
                row = (lax.broadcasted_iota(jnp.int32, (G * PR, CH), 0) & (PR - 1)) + (2 * pair + t) * PR
                s = jnp.where(key <= row, scores(pqs[t], c * CH), NEG)
                p, factor = soft(s, pm, t)
                pa[t] = pa[t] * both(factor) + mixed(p, c * CH)

    def answer(t, carry):
        n = jnp.where(t == 0, counts[0], counts[1])
        def where_is(u):
            c = u >> 3
            return pl.multiple_of(jnp.where(c < base // CH, c * CH, c * CH + t * span), CH)
        def stage_a(u, s):
            s[...] = scores(qs[t * G + (u & 7)], where_is(u))
        def stage_b(u, s, p, f, masked):
            x = s[...]
            if masked:
                key = lax.broadcasted_iota(jnp.int32, (RB, CH), 1) + ((u >> 3) * CH - base)
                row = lax.broadcasted_iota(jnp.int32, (RB, CH), 0) + (n - 1) * RB
                x = jnp.where(key <= row, x, NEG)
            p[...], f[...] = soft(x, m, t * G + (u & 7))
        def stage_c(u, p, f):
            i = t * G + (u & 7)
            a[i] = a[i] * both(f[...]) + mixed(p[...], where_is(u))
        def run(lo, hi, masked):
            stage_a(lo, s0)
            p1[...] = jnp.zeros(p1.shape, p1.dtype)
            f1[...] = jnp.ones(f1.shape, f1.dtype)
            def two(i, c):
                u = lo + 2 * i
                stage_a(u + 1, s1)
                stage_b(u, s0, p0, f0, masked)
                stage_c(jnp.maximum(u - 1, lo), p1, f1)
                stage_a(jnp.minimum(u + 2, hi - 1), s0)
                stage_b(u + 1, s1, p1, f1, masked)
                stage_c(u, p0, f0)
                return c
            lax.fori_loop(0, (hi - lo) // 2, two, 0)
            stage_c(hi - 1, p1, f1)
        plain = base // CH + (n - 1) * RB // CH
        every = base // CH + (n * RB + CH - 1) // CH
        lax.fori_loop(0, n, lambda i, c: (landed(t, i), c)[1], 0)
        run(0, plain * G, False)
        run(plain * G, every * G, True)
        return carry
    lax.fori_loop(0, 2, answer, 0)

    parts = out_ref.shape[0] // 2
    pn, rn = PR // parts, RB // parts
    for t in range(2):
        for h in range(G):
            cols = slice(h * D, (h + 1) * D)
            i = t * G + h
            done = (a[i, :, :D] / a[i, :, D:]).astype(jnp.bfloat16)
            rr = slice(h * PR, (h + 1) * PR)
            asked = (pa[t, rr, :D] / pa[t, rr, D:]).astype(jnp.bfloat16)
            for d in range(parts):
                out_ref[2 * d + t, :pn, cols] = asked[d * pn:(d + 1) * pn]
                out_ref[2 * d + t, pn:, cols] = done[d * rn:(d + 1) * rn]


def attention(place, lengths, table, own, got, pieces, parts):
    slots = table.shape[0]
    longest = slots // 2
    f32, bf16 = jnp.float32, jnp.bfloat16
    smem = pl.BlockSpec(memory_space=pltpu.SMEM)
    vmem = pl.BlockSpec(memory_space=pltpu.VMEM)
    return pl.pallas_call(
        functools.partial(kernel, slots=slots, members=lengths.shape[0], longest=longest),
        out_shape=jax.ShapeDtypeStruct((2 * parts, (PR + RB) // parts, own.shape[1]), bf16),
        in_specs=[smem, smem, smem, vmem, vmem] + [pl.BlockSpec(memory_space=pltpu.HBM)] * len(pieces),
        out_specs=vmem,
        scratch_shapes=[
            pltpu.SMEM((2 * longest,), jnp.int32),
            pltpu.VMEM((slots * PR + 2 * longest * RB, 3 * D), bf16),
            pltpu.VMEM((2 * G, RB, D), bf16),
            pltpu.VMEM((2, G * PR, D), bf16),
            pltpu.VMEM((2 * G, RB, D), f32), pltpu.VMEM((2 * G, RB, 2 * D), f32),
            pltpu.VMEM((2, G * PR, D), f32), pltpu.VMEM((2, G * PR, 2 * D), f32),
            pltpu.VMEM((RB, CH), f32), pltpu.VMEM((RB, CH), f32),
            pltpu.VMEM((RB, CH), bf16), pltpu.VMEM((RB, CH), bf16),
            pltpu.VMEM((RB, D), f32), pltpu.VMEM((RB, D), f32),
            pltpu.SemaphoreType.DMA, pltpu.SemaphoreType.DMA((2 * longest,)),
        ],
        compiler_params=pltpu.CompilerParams(vmem_limit_bytes=56 * 2**20),
        name="attention",
    )(place, lengths, table, own, got, *pieces)


SEQ = ("x", "y", "zp", "zq")
HEAD = ("zh", "core")


def on_device(pq, pk, pv, rq, rk, rv, lengths, table):
    side = lax.axis_index("zq").astype(jnp.int32)
    place = jnp.stack([lax.axis_index(n).astype(jnp.int32) for n in SEQ])
    half = rq.shape[1] // 2
    queries = jnp.concatenate([pq, rq], axis=0)
    give = lax.dynamic_slice_in_dim(queries, (1 - side) * half, half, 1)
    keep = lax.dynamic_slice_in_dim(queries, side * half, half, 1)
    keyval = jnp.stack(
        [jnp.concatenate([jnp.concatenate([p[:, j * D:(j + 1) * D], r[:, j * D:(j + 1) * D]], axis=0)
                          for p, r in ((pk, rk), (pv, rv))], axis=1) for j in range(2)])
    here = lax.dynamic_index_in_dim(keyval, side, 0, keepdims=False)
    there = lax.dynamic_index_in_dim(keyval, 1 - side, 0, keepdims=False)
    swap = [(0, 1), (1, 0)]
    next_to = lax.ppermute(there, "zq", swap)
    far_same = lax.ppermute(here, "zp", swap)
    far_other = lax.ppermute(there, ("zp", "zq"), [(i, 3 - i) for i in range(4)])

    def ring(t, axis):
        up, down = [(i, (i + 1) % 4) for i in range(4)], [(i, (i - 1) % 4) for i in range(4)]
        before, after = lax.ppermute(t, axis, up), lax.ppermute(t, axis, down)
        n = t.shape[0] // 2
        return t, before, after, lax.ppermute(before[:n], axis, up), lax.ppermute(after[n:], axis, down)

    def colour(t, first, second):
        own, before, after, half_a, half_b = ring(t, first)
        return ring(jnp.stack([own, after, jnp.concatenate([half_a, half_b], axis=0), before]), second)

    pieces = (colour(jnp.stack([here, next_to]), "x", "y")
              + colour(jnp.stack([far_same, far_other]), "y", "x"))
    got = lax.ppermute(give, "zq", swap)
    parts = lax.axis_size(HEAD)
    mixed = attention(place, lengths, table, keep, got, pieces, parts)
    back = lax.all_to_all(mixed, HEAD + ("zq",), split_axis=0, concat_axis=0, tiled=True)
    pn = PR // parts
    flat = lambda t: t.transpose(1, 0, 2).reshape(t.shape[1], -1)
    return flat(back[:, :pn]), flat(back[:, pn:])


def solution(mesh):
    grid = Mesh(mesh.devices.reshape(4, 4, 2, 2, 2, 2), SEQ + HEAD)
    both = P(SEQ, HEAD)
    rows = P(SEQ + HEAD, None)
    return jax.shard_map(
        on_device, mesh=grid, in_specs=(both,) * 6 + (P(), P()), out_specs=(rows, rows), check_vma=False
    )
```

```python
import functools

import jax
import jax.numpy as jnp
from jax import lax
from jax.experimental import pallas as pl
from jax.experimental.pallas import tpu as pltpu
from jax.sharding import Mesh, PartitionSpec as P

D = 128
RB = 192
PR = 32
G = 8
MH = 2
CH = 512
LIMIT = 36 * 2**20
PER_EXP = 128 ** -0.5 * 1.4426950408889634
NEG = -1e30
RING = (((0, 0, 4),), ((3, 0, 4), (1, 0, 4)), ((2, 0, 2), (2, 2, 2)))


def homes_of(groups):
    return [(colour, *h) for g in groups for colour in range(2) for h in RING[g]]


def kernel(place_ref, tab_ref, own_ref, got_ref, *refs, groups, last, region):
    first = 0 in groups
    homes = homes_of(groups)
    pieces, refs = refs[:len(homes)], refs[len(homes):]
    if not first:
        before, refs = refs[:4], refs[4:]
    if last:
        out_ref, refs = refs[0], refs[1:]
    m, a, pm, pa, kv, flags, qs, pqs, s0, s1, p0, p1, f0, f1 = refs
    px, py, pp, side = [place_ref[i] for i in range(4)]
    pair = (px * 4 + py) * 2 + pp
    width = 2 * D
    prompts = sum(2 * n * PR for _, _, _, n in homes)
    per = G // MH

    spans = [(place_ref[4 + t], place_ref[6 + t]) for t in range(2)]
    flags[:CH] = jnp.ones((CH, D), jnp.bfloat16)
    flags[CH:] = jnp.zeros((CH, D), jnp.bfloat16)

    def block(piece, r, t, i):
        kv[pl.ds(pl.multiple_of(t * region + prompts + i * RB, 64), RB), :] = piece[r, PR:, :]

    counts = (jnp.int32(0), jnp.int32(0))
    at = 0
    for piece, (colour, far, lead, n) in zip(pieces, homes):
        def bring(i, counts, piece=piece, colour=colour, far=far, lead=lead, at=at):
            near, e = i >> 1, i & 1
            dx, dy = (lead + near, far) if colour == 0 else (far, lead + near)
            slot = ((((px + dx) & 3) * 4 + ((py + dy) & 3)) * 2 + (pp ^ colour)) * 2 + (side ^ e)
            g = tab_ref[slot]
            new = []
            for t in range(2):
                kv[pl.ds(pl.multiple_of(t * region + (at + i) * PR, PR), PR), :] = piece[i, :PR, :]
                own, start = spans[t]
                hit = (g >= start) & (g < own)
                @pl.when(hit)
                def fetch(t=t):
                    block(piece, i, t, counts[t])
                new.append(counts[t] + hit.astype(jnp.int32))
            return tuple(new)
        counts = lax.fori_loop(0, 2 * n, bring, counts)
        at += 2 * n
    if first:
        for t in range(2):
            block(pieces[0], side ^ t, t, counts[t])
        counts = tuple(c + 1 for c in counts)
    keys = [prompts + c * RB for c in counts]
    chunks = [(k + CH - 1) // CH for k in keys]

    for src, t in ((own_ref, side), (got_ref, 1 - side)):
        for h in range(G):
            cols = slice(h * D, (h + 1) * D)
            qs[t * per + h // MH, pl.ds(h % MH * RB, RB)] = src[PR:, cols]
            pqs[pl.ds((t * G + h) * PR, PR)] = src[:PR, cols]
    if first:
        for r in (m, pm):
            r[...] = jnp.full(r.shape, NEG, jnp.float32)
        for r in (a, pa):
            r[...] = jnp.zeros(r.shape, jnp.float32)
    else:
        for r, b in zip((m, a, pm, pa), before):
            r[...] = b[...]
    for t in range(2):
        def pad(i, c, t=t):
            rows = pl.ds(pl.multiple_of(t * region + i * 64, 64), 64)
            kv[rows, :D] = kv[pl.ds(t * region, 64), :D]
            kv[rows, D:] = jnp.zeros((64, D), jnp.bfloat16)
            return c
        lax.fori_loop(keys[t] // 64, chunks[t] * (CH // 64), pad, 0)

    def soft(s, m_ref, i):
        old = m_ref[i]
        new = jnp.maximum(old, jnp.max(s, axis=1, keepdims=True))
        m_ref[i] = new
        spread = jnp.concatenate([new] * (s.shape[1] // D), axis=1)
        return jnp.exp2((s - spread) * PER_EXP).astype(jnp.bfloat16), jnp.exp2((old - new) * PER_EXP)

    def scores(q, start, n):
        return lax.dot_general(q, kv[pl.ds(start, n), :D], (((1,), (1,)), ((), ())), preferred_element_type=jnp.float32)

    def mixed(p, start, n, flag):
        v = jnp.concatenate([kv[pl.ds(start, n), D:], flag], axis=1)
        return lax.dot_general(p, v, (((1,), (0,)), ((), ())), preferred_element_type=jnp.float32)

    def both(f):
        return jnp.concatenate([f, f], axis=1)

    where = []
    for colour, far, lead, n in homes:
        lane = lax.broadcasted_iota(jnp.int32, (1, 2 * n * PR), 1)
        near, e = lead + (lane >> 6), (lane >> 5) & 1
        dx, dy = (near, jnp.int32(far)) if colour == 0 else (jnp.int32(far), near)
        slot = ((((px + dx) & 3) * 4 + ((py + dy) & 3)) * 2 + (pp ^ colour)) * 2 + (side ^ e)
        where.append(slot * PR + (lane & (PR - 1)))
    where = jnp.concatenate(where, axis=1)
    half = G * PR
    for t in range(2):
        row = (lax.broadcasted_iota(jnp.int32, (half, 1), 0) & (PR - 1)) + (2 * pair + t) * PR
        s = jnp.where(where <= row, scores(pqs[t * half:(t + 1) * half], 0, prompts), NEG)
        p, factor = soft(s, pm, t)
        pa[t] = pa[t] * both(factor) + mixed(p, 0, prompts, jnp.ones((prompts, D), jnp.bfloat16))

    split, total = chunks[0] * per, (chunks[0] + chunks[1]) * per
    shift = per.bit_length() - 1

    def unit(u):
        t = (u >= split).astype(jnp.int32)
        v = u - t * split
        c, h = v >> shift, v & (per - 1)
        return t, c, t * per + h, pl.multiple_of(t * region + c * CH, CH)

    def stage_a(u, s):
        _, _, i, start = unit(u)
        s[...] = scores(qs[i], start, CH)

    def stage_b(u, s, p, f):
        t, c, i, _ = unit(u)
        x = s[...]
        if first:
            key = lax.broadcasted_iota(jnp.int32, (MH * RB, CH), 1)
            row = lax.broadcasted_iota(jnp.int32, (MH * RB, 1), 0)
            row = jnp.where(row < RB, row, row - RB) + (jnp.where(t == 0, keys[0], keys[1]) - RB - c * CH)
            x = jnp.where(key <= row, x, NEG)
        p[...], f[...] = soft(x, m, i)

    def stage_c(u, p, f):
        t, c, i, start = unit(u)
        live = jnp.minimum(jnp.where(t == 0, keys[0], keys[1]) - c * CH, CH)
        flag = flags[pl.ds(pl.multiple_of(CH - live, 64), CH), :]
        a[i] = a[i] * both(f[...]) + mixed(p[...], start, CH, flag)

    stage_a(0, s0)
    p1[...] = jnp.zeros(p1.shape, p1.dtype)
    f1[...] = jnp.ones(f1.shape, f1.dtype)

    def two(i, c):
        u = 2 * i
        stage_a(u + 1, s1)
        stage_b(u, s0, p0, f0)
        stage_c(jnp.maximum(u - 1, 0), p1, f1)
        stage_a(jnp.minimum(u + 2, total - 1), s0)
        stage_b(u + 1, s1, p1, f1)
        stage_c(u, p0, f0)
        return c
    lax.fori_loop(0, total >> 1, two, 0)
    stage_c(total - 1, p1, f1)

    if last:
        parts = out_ref.shape[0] // 2
        pn, rn = PR // parts, RB // parts
        for t in range(2):
            for h in range(G):
                cols = slice(h * D, (h + 1) * D)
                i, top = t * per + h // MH, h % MH * RB
                done = (a[i, top:top + RB, :D] / a[i, top:top + RB, D:]).astype(jnp.bfloat16)
                rr = slice(h * PR, (h + 1) * PR)
                asked = (pa[t, rr, :D] / pa[t, rr, D:]).astype(jnp.bfloat16)
                for d in range(parts):
                    out_ref[2 * d + t, :pn, cols] = asked[d * pn:(d + 1) * pn]
                    out_ref[2 * d + t, pn:, cols] = done[d * rn:(d + 1) * rn]


def attention(place, table, own, got, pieces, state, groups, parts):
    slots = table.shape[0]
    f32, bf16 = jnp.float32, jnp.bfloat16
    smem = pl.BlockSpec(memory_space=pltpu.SMEM)
    vmem = pl.BlockSpec(memory_space=pltpu.VMEM)
    last = 2 in groups
    count = sum(2 * n for *_, n in homes_of(groups))
    region = -(-(count * PR + min(count, slots // 2) * RB) // CH) * CH
    units = 2 * G // MH
    shapes = [(units, MH * RB, D), (units, MH * RB, 2 * D), (2, G * PR, D), (2, G * PR, 2 * D)]
    inputs = [place, table, own, got, *pieces, *state]
    kept = [jax.ShapeDtypeStruct(s, f32) for s in shapes]
    if last:
        out_shape, out_specs = jax.ShapeDtypeStruct((2 * parts, (PR + RB) // parts, G * D), bf16), vmem
    else:
        out_shape, out_specs = kept, [vmem] * 4
    flops = 4 * RB * G * 2 * D * (count * (PR + RB // 2))
    return pl.pallas_call(
        functools.partial(kernel, groups=groups, last=last, region=region),
        out_shape=out_shape,
        in_specs=[smem, smem] + [vmem] * (len(inputs) - 2),
        out_specs=out_specs,
        scratch_shapes=([pltpu.VMEM(s, f32) for s in shapes] if last else []) + [
            pltpu.VMEM((2 * region, 2 * D), bf16),
            pltpu.VMEM((2 * CH, D), bf16),
            pltpu.VMEM((units, MH * RB, D), bf16),
            pltpu.VMEM((2 * G * PR, D), bf16),
            pltpu.VMEM((MH * RB, CH), f32), pltpu.VMEM((MH * RB, CH), f32),
            pltpu.VMEM((MH * RB, CH), bf16), pltpu.VMEM((MH * RB, CH), bf16),
            pltpu.VMEM((MH * RB, D), f32), pltpu.VMEM((MH * RB, D), f32),
        ],
        cost_estimate=pl.CostEstimate(flops=flops, transcendentals=flops // 512, bytes_accessed=2**23),
        compiler_params=pltpu.CompilerParams(vmem_limit_bytes=LIMIT),
        name="attention",
    )(*inputs)


def attend(place, table, own, got, gathered, parts):
    gathered = [[p.reshape(-1, *p.shape[2:]) for p in c] for c in gathered]
    run = functools.partial(attention, place, table, own, got)
    state = run([c[0] for c in gathered], (), (0,), parts)
    state = run([p for c in gathered for p in c[1:3]], state, (1,), parts)
    return run([p for c in gathered for p in c[3:]], state, (2,), parts)


SEQ = ("x", "y", "zp", "zq")
HEAD = ("zh", "core")


def on_device(pq, pk, pv, rq, rk, rv, lengths, table):
    side = lax.axis_index("zq").astype(jnp.int32)
    place = [lax.axis_index(n).astype(jnp.int32) for n in SEQ]
    mates = lax.dynamic_slice_in_dim(table, (place[0] * 4 + place[1]) * 4 + place[2] * 2, 2, 0)
    ends = jnp.cumsum(lengths)
    begun = jnp.where(mates[:, None] >= ends[None, :], ends[None, :], 0)
    place = jnp.concatenate([jnp.stack(place), mates, jnp.max(begun, axis=1)])
    half = rq.shape[1] // 2
    queries = jnp.concatenate([pq, rq], axis=0)
    give = lax.dynamic_slice_in_dim(queries, (1 - side) * half, half, 1)
    keep = lax.dynamic_slice_in_dim(queries, side * half, half, 1)
    keyval = jnp.stack(
        [jnp.concatenate([jnp.concatenate([p[:, j * D:(j + 1) * D], r[:, j * D:(j + 1) * D]], axis=0)
                          for p, r in ((pk, rk), (pv, rv))], axis=1) for j in range(2)])
    here = lax.dynamic_index_in_dim(keyval, side, 0, keepdims=False)
    there = lax.dynamic_index_in_dim(keyval, 1 - side, 0, keepdims=False)
    swap = [(0, 1), (1, 0)]
    next_to = lax.ppermute(there, "zq", swap)
    far_same = lax.ppermute(here, "zp", swap)
    far_other = lax.ppermute(there, ("zp", "zq"), [(i, 3 - i) for i in range(4)])

    def ring(t, axis):
        up, down = [(i, (i + 1) % 4) for i in range(4)], [(i, (i - 1) % 4) for i in range(4)]
        before, after = lax.ppermute(t, axis, up), lax.ppermute(t, axis, down)
        n = t.shape[0] // 2
        return t, before, after, lax.ppermute(before[:n], axis, up), lax.ppermute(after[n:], axis, down)

    def colour(t, first, second):
        own, before, after, half_a, half_b = ring(t, first)
        return ring(jnp.stack([own, after, jnp.concatenate([half_a, half_b], axis=0), before]), second)

    gathered = (colour(jnp.stack([here, next_to]), "x", "y"), colour(jnp.stack([far_same, far_other]), "y", "x"))
    got = lax.ppermute(give, "zq", swap)
    parts = lax.axis_size(HEAD)
    mixed = attend(place, table, keep, got, gathered, parts)
    back = lax.all_to_all(mixed, HEAD + ("zq",), split_axis=0, concat_axis=0, tiled=True)
    pn = PR // parts
    flat = lambda t: t.transpose(1, 0, 2).reshape(t.shape[1], -1)
    return flat(back[:, :pn]), flat(back[:, pn:])


def solution(mesh):
    grid = Mesh(mesh.devices.reshape(4, 4, 2, 2, 2, 2), SEQ + HEAD)
    both = P(SEQ, HEAD)
    rows = P(SEQ + HEAD, None)
    return jax.shard_map(
        on_device, mesh=grid, in_specs=(both,) * 6 + (P(), P()), out_specs=(rows, rows), check_vma=False
    )
```

```python
import functools

import jax
import jax.numpy as jnp
from jax import lax
from jax.experimental import pallas as pl
from jax.experimental.pallas import tpu as pltpu
from jax.sharding import Mesh, PartitionSpec as P


D = 128
RB = 192
PR = 32
G = 8
CH = 512
LIMIT = 36 * 2**20
PER_EXP = 128 ** -0.5 * 1.4426950408889634
NEG = -1e30
RING = (((0, 0, 4),), ((3, 0, 4), (1, 0, 4)), ((2, 0, 2), (2, 2, 2)))


def homes_of(groups):
    return [(colour, *h) for g in groups for colour in range(2) for h in RING[g]]


def kernel(place_ref, tab_ref, own_ref, got_ref, *refs, groups, last, region, mh):
    first = 0 in groups
    homes = homes_of(groups)
    pieces, refs = refs[:len(homes)], refs[len(homes):]
    if not first:
        before, refs = refs[:4], refs[4:]
    if last:
        out_ref, refs = refs[0], refs[1:]
    m, a, pm, pa, kv, flags, qs, pqs, s0, s1, p0, p1, f0, f1 = refs
    px, py, pp, side = [place_ref[i] for i in range(4)]
    pair = (px * 4 + py) * 2 + pp
    prompts = sum(2 * n * PR for _, _, _, n in homes)
    per = G // mh

    spans = [(place_ref[4 + t], place_ref[6 + t]) for t in range(2)]
    flags[:CH] = jnp.ones((CH, D), jnp.bfloat16)
    flags[CH:] = jnp.zeros((CH, D), jnp.bfloat16)

    def block(piece, r, t, i):
        kv[pl.ds(pl.multiple_of(t * region + prompts + i * RB, 64), RB), :] = piece[r, PR:, :]

    counts = (jnp.int32(0), jnp.int32(0))
    at = 0
    for piece, (colour, far, lead, n) in zip(pieces, homes):
        def bring(i, counts, piece=piece, colour=colour, far=far, lead=lead, at=at):
            near, e = i >> 1, i & 1
            dx, dy = (lead + near, far) if colour == 0 else (far, lead + near)
            slot = ((((px + dx) & 3) * 4 + ((py + dy) & 3)) * 2 + (pp ^ colour)) * 2 + (side ^ e)
            g = tab_ref[slot]
            new = []
            for t in range(2):
                kv[pl.ds(pl.multiple_of(t * region + (at + i) * PR, PR), PR), :] = piece[i, :PR, :]
                own, start = spans[t]
                hit = (g >= start) & (g < own)

                @pl.when(hit)
                def fetch(t=t):
                    block(piece, i, t, counts[t])

                new.append(counts[t] + hit.astype(jnp.int32))
            return tuple(new)

        counts = lax.fori_loop(0, 2 * n, bring, counts)
        at += 2 * n
    if first:
        for t in range(2):
            block(pieces[0], side ^ t, t, counts[t])
        counts = tuple(c + 1 for c in counts)
    keys = [prompts + c * RB for c in counts]
    chunks = [(k + CH - 1) // CH for k in keys]

    for src, t in ((own_ref, side), (got_ref, 1 - side)):
        for h in range(G):
            cols = slice(h * D, (h + 1) * D)
            qs[t * per + h // mh, pl.ds(h % mh * RB, RB)] = src[PR:, cols]
            pqs[pl.ds((t * G + h) * PR, PR)] = src[:PR, cols]
    if first:
        for r in (m, pm):
            r[...] = jnp.full(r.shape, NEG, jnp.float32)
        for r in (a, pa):
            r[...] = jnp.zeros(r.shape, jnp.float32)
    else:
        for r, b in zip((m, a, pm, pa), before):
            r[...] = b[...]
    for t in range(2):
        def pad(i, c, t=t):
            rows = pl.ds(pl.multiple_of(t * region + i * 64, 64), 64)
            kv[rows, :D] = kv[pl.ds(t * region, 64), :D]
            kv[rows, D:] = jnp.zeros((64, D), jnp.bfloat16)
            return c

        lax.fori_loop(keys[t] // 64, chunks[t] * (CH // 64), pad, 0)

    def soft(s, m_ref, i):
        old = m_ref[i]
        new = jnp.maximum(old, jnp.max(s, axis=1, keepdims=True))
        m_ref[i] = new
        spread = jnp.concatenate([new] * (s.shape[1] // D), axis=1)
        return jnp.exp2((s - spread) * PER_EXP).astype(jnp.bfloat16), jnp.exp2((old - new) * PER_EXP)

    def scores(q, start, n):
        return lax.dot_general(q, kv[pl.ds(start, n), :D], (((1,), (1,)), ((), ())), preferred_element_type=jnp.float32)

    def mixed(p, start, n, flag):
        v = jnp.concatenate([kv[pl.ds(start, n), D:], flag], axis=1)
        return lax.dot_general(p, v, (((1,), (0,)), ((), ())), preferred_element_type=jnp.float32)

    def both(f):
        return jnp.concatenate([f, f], axis=1)

    where = []
    for colour, far, lead, n in homes:
        lane = lax.broadcasted_iota(jnp.int32, (1, 2 * n * PR), 1)
        near, e = lead + (lane >> 6), (lane >> 5) & 1
        dx, dy = (near, jnp.int32(far)) if colour == 0 else (jnp.int32(far), near)
        slot = ((((px + dx) & 3) * 4 + ((py + dy) & 3)) * 2 + (pp ^ colour)) * 2 + (side ^ e)
        where.append(slot * PR + (lane & (PR - 1)))
    where = jnp.concatenate(where, axis=1)
    half = G * PR
    for t in range(2):
        row = (lax.broadcasted_iota(jnp.int32, (half, 1), 0) & (PR - 1)) + (2 * pair + t) * PR
        s = jnp.where(where <= row, scores(pqs[t * half:(t + 1) * half], 0, prompts), NEG)
        p, factor = soft(s, pm, t)
        pa[t] = pa[t] * both(factor) + mixed(p, 0, prompts, jnp.ones((prompts, D), jnp.bfloat16))

    split, total = chunks[0] * per, (chunks[0] + chunks[1]) * per
    shift = per.bit_length() - 1

    def unit(u):
        t = (u >= split).astype(jnp.int32)
        v = u - t * split
        c, h = v >> shift, v & (per - 1)
        return t, c, t * per + h, pl.multiple_of(t * region + c * CH, CH)

    def stage_a(u, s):
        _, _, i, start = unit(u)
        s[...] = scores(qs[i], start, CH)

    def stage_b(u, s, p, f):
        t, c, i, _ = unit(u)
        x = s[...]
        if first:
            key = lax.broadcasted_iota(jnp.int32, (mh * RB, CH), 1)
            row = lax.broadcasted_iota(jnp.int32, (mh * RB, 1), 0)
            row = row % RB + (jnp.where(t == 0, keys[0], keys[1]) - RB - c * CH)
            x = jnp.where(key <= row, x, NEG)
        p[...], f[...] = soft(x, m, i)

    def stage_c(u, p, f):
        t, c, i, start = unit(u)
        live = jnp.minimum(jnp.where(t == 0, keys[0], keys[1]) - c * CH, CH)
        flag = flags[pl.ds(pl.multiple_of(CH - live, 64), CH), :]
        a[i] = a[i] * both(f[...]) + mixed(p[...], start, CH, flag)

    stage_a(0, s0)
    p1[...] = jnp.zeros(p1.shape, p1.dtype)
    f1[...] = jnp.ones(f1.shape, f1.dtype)

    def two(i, c):
        u = 2 * i
        stage_a(u + 1, s1)
        stage_b(u, s0, p0, f0)
        stage_c(jnp.maximum(u - 1, 0), p1, f1)
        stage_a(jnp.minimum(u + 2, total - 1), s0)
        stage_b(u + 1, s1, p1, f1)
        stage_c(u, p0, f0)
        return c

    lax.fori_loop(0, total >> 1, two, 0)
    stage_c(total - 1, p1, f1)

    if last:
        parts = out_ref.shape[0] // 2
        pn, rn = PR // parts, RB // parts
        for t in range(2):
            for h in range(G):
                cols = slice(h * D, (h + 1) * D)
                i, top = t * per + h // mh, h % mh * RB
                done = (a[i, top:top + RB, :D] / a[i, top:top + RB, D:]).astype(jnp.bfloat16)
                rr = slice(h * PR, (h + 1) * PR)
                asked = (pa[t, rr, :D] / pa[t, rr, D:]).astype(jnp.bfloat16)
                for d in range(parts):
                    out_ref[2 * d + t, :pn, cols] = asked[d * pn:(d + 1) * pn]
                    out_ref[2 * d + t, pn:, cols] = done[d * rn:(d + 1) * rn]


def attention(place, table, own, got, pieces, state, groups, parts, mh):
    slots = table.shape[0]
    f32, bf16 = jnp.float32, jnp.bfloat16
    smem = pl.BlockSpec(memory_space=pltpu.SMEM)
    vmem = pl.BlockSpec(memory_space=pltpu.VMEM)
    last = 2 in groups
    count = sum(2 * n for *_, n in homes_of(groups))
    region = -(-(count * PR + min(count, slots // 2) * RB) // CH) * CH
    units = 2 * G // mh
    shapes = [(units, mh * RB, D), (units, mh * RB, 2 * D), (2, G * PR, D), (2, G * PR, 2 * D)]
    state = [x.reshape(shape) for x, shape in zip(state, shapes)]
    inputs = [place, table, own, got, *pieces, *state]
    kept = [jax.ShapeDtypeStruct(s, f32) for s in shapes]
    if last:
        out_shape, out_specs = jax.ShapeDtypeStruct((2 * parts, (PR + RB) // parts, G * D), bf16), vmem
    else:
        out_shape, out_specs = kept, [vmem] * 4
    flops = 4 * RB * G * 2 * D * (count * (PR + RB // 2))
    return pl.pallas_call(
        functools.partial(kernel, groups=groups, last=last, region=region, mh=mh),
        out_shape=out_shape,
        in_specs=[smem, smem] + [vmem] * (len(inputs) - 2),
        out_specs=out_specs,
        scratch_shapes=([pltpu.VMEM(s, f32) for s in shapes] if last else []) + [
            pltpu.VMEM((2 * region, 2 * D), bf16),
            pltpu.VMEM((2 * CH, D), bf16),
            pltpu.VMEM((units, mh * RB, D), bf16),
            pltpu.VMEM((2 * G * PR, D), bf16),
            pltpu.VMEM((mh * RB, CH), f32), pltpu.VMEM((mh * RB, CH), f32),
            pltpu.VMEM((mh * RB, CH), bf16), pltpu.VMEM((mh * RB, CH), bf16),
            pltpu.VMEM((mh * RB, D), f32), pltpu.VMEM((mh * RB, D), f32),
        ],
        cost_estimate=pl.CostEstimate(flops=flops, transcendentals=flops // 512, bytes_accessed=2**23),
        compiler_params=pltpu.CompilerParams(vmem_limit_bytes=LIMIT),
        name="attention",
    )(*inputs)


def attend(place, table, own, got, gathered, parts):
    gathered = [[p.reshape(-1, *p.shape[2:]) for p in c] for c in gathered]
    run = functools.partial(attention, place, table, own, got)
    state = run([c[0] for c in gathered], (), (0,), parts, 2)
    state = run([p for c in gathered for p in c[1:3]], state, (1,), parts, 4)
    return run([p for c in gathered for p in c[3:]], state, (2,), parts, 4)


def together(copies):
    for c in copies:
        c.start()
    for c in copies:
        c.wait()


def sort_keys(side_ref, pk, pv, rk, rv, here, there, sems):
    side = side_ref[0]
    copies = []
    for out, j in ((here, side), (there, 1 - side)):
        for rows, k, v in ((pl.ds(0, PR), pk, pv), (pl.ds(PR, RB), rk, rv)):
            for w, src in enumerate((k, v)):
                copies.append(pltpu.make_async_copy(
                    src.at[:, pl.ds(pl.multiple_of(j * D, D), D)], out.at[rows, pl.ds(w * D, D)], sems.at[len(copies)]))
    together(copies)


def sort_queries(side_ref, pq, rq, keep, give, sems):
    side, half = side_ref[0], keep.shape[1]
    copies = []
    for out, j in ((keep, side), (give, 1 - side)):
        for rows, src in ((pl.ds(0, PR), pq), (pl.ds(PR, RB), rq)):
            copies.append(pltpu.make_async_copy(
                src.at[:, pl.ds(pl.multiple_of(j * half, half), half)], out.at[rows], sems.at[len(copies)]))
    together(copies)


def sorted_by_side(body, side, arrays, cols):
    out = jax.ShapeDtypeStruct((PR + RB, cols), jnp.bfloat16)
    vmem = pl.BlockSpec(memory_space=pltpu.VMEM)
    return pl.pallas_call(
        body, out_shape=(out, out),
        in_specs=[pl.BlockSpec(memory_space=pltpu.SMEM)] + [pl.BlockSpec(memory_space=pltpu.HBM)] * len(arrays),
        out_specs=(vmem, vmem), scratch_shapes=[pltpu.SemaphoreType.DMA((2 * len(arrays),))],
        compiler_params=pltpu.CompilerParams(vmem_limit_bytes=8 * 2**20),
    )(side.reshape(1), *arrays)


SEQ = ("x", "y", "zp", "zq")
HEAD = ("zh", "core")


def whole(pq, pk, pv, rq, rk, rv, lengths, table):
    side = lax.axis_index("zq").astype(jnp.int32)
    place = [lax.axis_index(n).astype(jnp.int32) for n in SEQ]
    mates = lax.dynamic_slice_in_dim(table, (place[0] * 4 + place[1]) * 4 + place[2] * 2, 2, 0)
    ends = jnp.cumsum(lengths)
    begun = jnp.where(mates[:, None] >= ends[None, :], ends[None, :], 0)
    place = jnp.concatenate([jnp.stack(place), mates, jnp.max(begun, axis=1)])
    here, there = sorted_by_side(sort_keys, side, (pk, pv, rk, rv), 2 * D)
    keep, give = sorted_by_side(sort_queries, side, (pq, rq), rq.shape[1] // 2)
    swap = [(0, 1), (1, 0)]
    next_to = lax.ppermute(there, "zq", swap)
    far_same = lax.ppermute(here, "zp", swap)
    far_other = lax.ppermute(there, ("zp", "zq"), [(i, 3 - i) for i in range(4)])

    far_other, give = lax.optimization_barrier((far_other, give))
    got = lax.ppermute(give, "zq", swap)

    def ring(t, axis):
        up, down = [(i, (i + 1) % 4) for i in range(4)], [(i, (i - 1) % 4) for i in range(4)]
        before, after = lax.ppermute(t, axis, up), lax.ppermute(t, axis, down)
        n = t.shape[0] // 2
        return t, before, after, lax.ppermute(before[:n], axis, up), lax.ppermute(after[n:], axis, down)

    def colour(t, first, second):
        own, before, after, half_a, half_b = ring(t, first)
        return ring(jnp.stack([own, after, jnp.concatenate([half_a, half_b], axis=0), before]), second)

    gathered = (colour(jnp.stack([here, next_to]), "x", "y"), colour(jnp.stack([far_same, far_other]), "y", "x"))
    parts = lax.axis_size(HEAD)
    mixed = attend(place, table, keep, got, gathered, parts)
    back = lax.all_to_all(mixed, HEAD + ("zq",), split_axis=0, concat_axis=0, tiled=True)
    pn = PR // parts
    flat = lambda t: t.transpose(1, 0, 2).reshape(t.shape[1], -1)
    return flat(back[:, :pn]), flat(back[:, pn:])


def solution(mesh):
    grid = Mesh(mesh.devices.reshape(4, 4, 2, 2, 2, 2), SEQ + HEAD)
    both = P(SEQ, HEAD)
    rows = P(SEQ + HEAD, None)
    return jax.shard_map(whole, mesh=grid, in_specs=(both,) * 6 + (P(), P()), out_specs=(rows, rows), check_vma=False)
```

```python
import functools

import jax
import jax.numpy as jnp
from jax import lax
from jax.experimental import pallas as pl
from jax.experimental.pallas import tpu as pltpu
from jax.sharding import Mesh, PartitionSpec as P


D = 128
RB = 192
PR = 32
G = 8
CH = 512
LIMIT = 36 * 2**20
PER_EXP = 128 ** -0.5 * 1.4426950408889634
NEG = -1e30
RING = (((0, 0, 4),), ((3, 0, 4), (1, 0, 4)), ((2, 0, 2), (2, 2, 2)))


def homes_of(groups):
    return [(colour, *h) for g in groups for colour in range(2) for h in RING[g]]


def kernel(place_ref, tab_ref, own_ref, got_ref, *refs, groups, last, region, mh, half):
    first = 0 in groups
    homes = homes_of(groups)
    pieces, refs = refs[:len(homes)], refs[len(homes):]
    if not first:
        before, refs = refs[:4], refs[4:]
    if last:
        outs, refs = refs[:2], refs[2:]
    m, a, pm, pa, kv, flags, qs, pqs, s0, s1, p0, p1, f0, f1 = refs
    px, py, pp, side = [place_ref[i] for i in range(4)]
    pair = (px * 4 + py) * 2 + pp
    prompts = sum(2 * n * PR for _, _, _, n in homes)
    nh, h0 = (G, 0) if half is None else (G // 2, half * (G // 2))
    per = nh // mh

    spans = [(place_ref[4 + t], place_ref[6 + t]) for t in range(2)]
    flags[:CH] = jnp.ones((CH, D), jnp.bfloat16)
    flags[CH:] = jnp.zeros((CH, D), jnp.bfloat16)

    def block(piece, r, t, i):
        kv[pl.ds(pl.multiple_of(t * region + prompts + i * RB, 64), RB), :] = piece[r, PR:, :]

    counts = (jnp.int32(0), jnp.int32(0))
    at = 0
    for piece, (colour, far, lead, n) in zip(pieces, homes):
        def bring(i, counts, piece=piece, colour=colour, far=far, lead=lead, at=at):
            near, e = i >> 1, i & 1
            dx, dy = (lead + near, far) if colour == 0 else (far, lead + near)
            slot = ((((px + dx) & 3) * 4 + ((py + dy) & 3)) * 2 + (pp ^ colour)) * 2 + (side ^ e)
            g = tab_ref[slot]
            new = []
            for t in range(2):
                kv[pl.ds(pl.multiple_of(t * region + (at + i) * PR, PR), PR), :] = piece[i, :PR, :]
                own, start = spans[t]
                hit = (g >= start) & (g < own)

                @pl.when(hit)
                def fetch(t=t):
                    block(piece, i, t, counts[t])

                new.append(counts[t] + hit.astype(jnp.int32))
            return tuple(new)

        counts = lax.fori_loop(0, 2 * n, bring, counts)
        at += 2 * n
    if first:
        for t in range(2):
            block(pieces[0], side ^ t, t, counts[t])
        counts = tuple(c + 1 for c in counts)
    keys = [prompts + c * RB for c in counts]
    chunks = [(k + CH - 1) // CH for k in keys]

    for src, t in ((own_ref, side), (got_ref, 1 - side)):
        for h in range(nh):
            cols = slice((h0 + h) * D, (h0 + h + 1) * D)
            qs[t * per + h // mh, pl.ds(h % mh * RB, RB)] = src[PR:, cols]
            pqs[pl.ds((t * nh + h) * PR, PR)] = src[:PR, cols]
    if first:
        for r in (m, pm):
            r[...] = jnp.full(r.shape, NEG, jnp.float32)
        for r in (a, pa):
            r[...] = jnp.zeros(r.shape, jnp.float32)
    elif half is None:
        for r, b in zip((m, a, pm, pa), before):
            r[...] = b[...]
    else:
        for t in range(2):
            for q in range(per):
                i, j = t * per + q, (2 * t + half) * per + q
                m[i], a[i] = before[0][j], before[1][j]
            pm[t], pa[t] = [b[t, half * nh * PR:(half + 1) * nh * PR] for b in before[2:]]
    for t in range(2):
        def pad(i, c, t=t):
            rows = pl.ds(pl.multiple_of(t * region + i * 64, 64), 64)
            kv[rows, :D] = kv[pl.ds(t * region, 64), :D]
            kv[rows, D:] = jnp.zeros((64, D), jnp.bfloat16)
            return c

        lax.fori_loop(keys[t] // 64, chunks[t] * (CH // 64), pad, 0)

    def soft(s, m_ref, i):
        old = m_ref[i]
        new = jnp.maximum(old, jnp.max(s, axis=1, keepdims=True))
        m_ref[i] = new
        spread = jnp.concatenate([new] * (s.shape[1] // D), axis=1)
        return jnp.exp2((s - spread) * PER_EXP).astype(jnp.bfloat16), jnp.exp2((old - new) * PER_EXP)

    def scores(q, start, n):
        return lax.dot_general(q, kv[pl.ds(start, n), :D], (((1,), (1,)), ((), ())), preferred_element_type=jnp.float32)

    def mixed(p, start, n, flag):
        v = jnp.concatenate([kv[pl.ds(start, n), D:], flag], axis=1)
        return lax.dot_general(p, v, (((1,), (0,)), ((), ())), preferred_element_type=jnp.float32)

    def both(f):
        return jnp.concatenate([f, f], axis=1)

    where = []
    for colour, far, lead, n in homes:
        lane = lax.broadcasted_iota(jnp.int32, (1, 2 * n * PR), 1)
        near, e = lead + (lane >> 6), (lane >> 5) & 1
        dx, dy = (near, jnp.int32(far)) if colour == 0 else (jnp.int32(far), near)
        slot = ((((px + dx) & 3) * 4 + ((py + dy) & 3)) * 2 + (pp ^ colour)) * 2 + (side ^ e)
        where.append(slot * PR + (lane & (PR - 1)))
    where = jnp.concatenate(where, axis=1)
    asked = nh * PR
    for t in range(2):
        row = (lax.broadcasted_iota(jnp.int32, (asked, 1), 0) & (PR - 1)) + (2 * pair + t) * PR
        s = jnp.where(where <= row, scores(pqs[t * asked:(t + 1) * asked], 0, prompts), NEG)
        p, factor = soft(s, pm, t)
        pa[t] = pa[t] * both(factor) + mixed(p, 0, prompts, jnp.ones((prompts, D), jnp.bfloat16))

    split, total = chunks[0] * per, (chunks[0] + chunks[1]) * per
    shift = per.bit_length() - 1

    def unit(u):
        t = (u >= split).astype(jnp.int32)
        v = u - t * split
        c, h = v >> shift, v & (per - 1)
        return t, c, t * per + h, pl.multiple_of(t * region + c * CH, CH)

    def stage_a(u, s):
        _, _, i, start = unit(u)
        s[...] = scores(qs[i], start, CH)

    def stage_b(u, s, p, f):
        t, c, i, _ = unit(u)
        x = s[...]
        if first:
            key = lax.broadcasted_iota(jnp.int32, (mh * RB, CH), 1)
            row = lax.broadcasted_iota(jnp.int32, (mh * RB, 1), 0)
            row = row % RB + (jnp.where(t == 0, keys[0], keys[1]) - RB - c * CH)
            x = jnp.where(key <= row, x, NEG)
        p[...], f[...] = soft(x, m, i)

    def stage_c(u, p, f):
        t, c, i, start = unit(u)
        live = jnp.minimum(jnp.where(t == 0, keys[0], keys[1]) - c * CH, CH)
        flag = flags[pl.ds(pl.multiple_of(CH - live, 64), CH), :]
        a[i] = a[i] * both(f[...]) + mixed(p[...], start, CH, flag)

    stage_a(0, s0)
    p1[...] = jnp.zeros(p1.shape, p1.dtype)
    f1[...] = jnp.ones(f1.shape, f1.dtype)

    def two(i, c):
        u = 2 * i
        stage_a(u + 1, s1)
        stage_b(u, s0, p0, f0)
        stage_c(jnp.maximum(u - 1, 0), p1, f1)
        stage_a(jnp.minimum(u + 2, total - 1), s0)
        stage_b(u + 1, s1, p1, f1)
        stage_c(u, p0, f0)
        return c

    lax.fori_loop(0, total >> 1, two, 0)
    stage_c(total - 1, p1, f1)

    if last:
        zh, n = place_ref[8], 2 * outs[0].shape[0] // 2
        pn, rn = PR // n, RB // n
        for t in range(2):
            for h in range(nh):
                cols = slice(h * D, (h + 1) * D)
                i, top = t * per + h // mh, h % mh * RB
                for k, out in enumerate(outs):
                    for core in range(2):
                        d = 2 * (zh ^ k) + core
                        rr = pl.ds(pl.multiple_of(h * PR + d * pn, 8), pn)
                        out[2 * core + t, :pn, cols] = (pa[t, rr, :D] / pa[t, rr, D:]).astype(jnp.bfloat16)
                        rr = pl.ds(pl.multiple_of(top + d * rn, 8), rn)
                        out[2 * core + t, pn:, cols] = (a[i, rr, :D] / a[i, rr, D:]).astype(jnp.bfloat16)


def attention(place, table, own, got, pieces, state, groups, parts, mh, half=None):
    slots = table.shape[0]
    f32, bf16 = jnp.float32, jnp.bfloat16
    smem = pl.BlockSpec(memory_space=pltpu.SMEM)
    vmem = pl.BlockSpec(memory_space=pltpu.VMEM)
    last = 2 in groups
    count = sum(2 * n for *_, n in homes_of(groups))
    region = -(-(count * PR + min(count, slots // 2) * RB) // CH) * CH

    def shapes_of(nh):
        units = 2 * nh // mh
        return [(units, mh * RB, D), (units, mh * RB, 2 * D), (2, nh * PR, D), (2, nh * PR, 2 * D)]

    nh = G if half is None else G // 2
    shapes, units = shapes_of(nh), 2 * nh // mh
    state = [x.reshape(shape) for x, shape in zip(state, shapes_of(G))]
    inputs = [place, table, own, got, *pieces, *state]
    kept = [jax.ShapeDtypeStruct(s, f32) for s in shapes]
    if last:
        out_shape, out_specs = (jax.ShapeDtypeStruct((parts, (PR + RB) // parts, nh * D), bf16),) * 2, (vmem, vmem)
    else:
        out_shape, out_specs = kept, [vmem] * 4
    flops = 4 * RB * nh * 2 * D * (count * (PR + RB // 2))
    return pl.pallas_call(
        functools.partial(kernel, groups=groups, last=last, region=region, mh=mh, half=half),
        out_shape=out_shape,
        in_specs=[smem, smem] + [vmem] * (len(inputs) - 2),
        out_specs=out_specs,
        scratch_shapes=([pltpu.VMEM(s, f32) for s in shapes] if last else []) + [
            pltpu.VMEM((2 * region, 2 * D), bf16),
            pltpu.VMEM((2 * CH, D), bf16),
            pltpu.VMEM((units, mh * RB, D), bf16),
            pltpu.VMEM((2 * nh * PR, D), bf16),
            pltpu.VMEM((mh * RB, CH), f32), pltpu.VMEM((mh * RB, CH), f32),
            pltpu.VMEM((mh * RB, CH), bf16), pltpu.VMEM((mh * RB, CH), bf16),
            pltpu.VMEM((mh * RB, D), f32), pltpu.VMEM((mh * RB, D), f32),
        ],
        cost_estimate=pl.CostEstimate(flops=flops, transcendentals=flops // 512, bytes_accessed=2**23),
        compiler_params=pltpu.CompilerParams(vmem_limit_bytes=LIMIT),
        name="attention",
    )(*inputs)


def attend(place, table, own, got, gathered, parts):
    gathered = [[p.reshape(-1, *p.shape[2:]) for p in c] for c in gathered]
    run = functools.partial(attention, place, table, own, got)
    state = run([c[0] for c in gathered], (), (0,), parts, 2)
    state = run([p for c in gathered for p in c[1:3]], state, (1,), parts, 4)
    return [run([p for c in gathered for p in c[3:]], state, (2,), parts, 2, half) for half in range(2)]


def together(copies):
    for c in copies:
        c.start()
    for c in copies:
        c.wait()


def sort_keys(side_ref, pk, pv, rk, rv, here, there, sems):
    side = side_ref[0]
    copies = []
    for out, j in ((here, side), (there, 1 - side)):
        for rows, k, v in ((pl.ds(0, PR), pk, pv), (pl.ds(PR, RB), rk, rv)):
            for w, src in enumerate((k, v)):
                copies.append(pltpu.make_async_copy(
                    src.at[:, pl.ds(pl.multiple_of(j * D, D), D)], out.at[rows, pl.ds(w * D, D)], sems.at[len(copies)]))
    together(copies)


def sort_queries(side_ref, pq, rq, keep, give, sems):
    side, half = side_ref[0], keep.shape[1]
    copies = []
    for out, j in ((keep, side), (give, 1 - side)):
        for rows, src in ((pl.ds(0, PR), pq), (pl.ds(PR, RB), rq)):
            copies.append(pltpu.make_async_copy(
                src.at[:, pl.ds(pl.multiple_of(j * half, half), half)], out.at[rows], sems.at[len(copies)]))
    together(copies)


def sorted_by_side(body, side, arrays, cols):
    out = jax.ShapeDtypeStruct((PR + RB, cols), jnp.bfloat16)
    vmem = pl.BlockSpec(memory_space=pltpu.VMEM)
    return pl.pallas_call(
        body, out_shape=(out, out),
        in_specs=[pl.BlockSpec(memory_space=pltpu.SMEM)] + [pl.BlockSpec(memory_space=pltpu.HBM)] * len(arrays),
        out_specs=(vmem, vmem), scratch_shapes=[pltpu.SemaphoreType.DMA((2 * len(arrays),))],
        compiler_params=pltpu.CompilerParams(vmem_limit_bytes=8 * 2**20),
    )(side.reshape(1), *arrays)


def set_columns(zh_ref, got, prompt_out, answer_out):
    pn, width = prompt_out.shape[0], got.shape[3]
    for zh in range(2):
        @pl.when(zh_ref[0] == zh)
        def write(zh=zh):
            for src in range(4):
                core, zq = src >> 1, src & 1
                for k in range(2):
                    block = ((zh ^ k) * 2 + core) * 2 + (zq ^ k)
                    for half in range(2):
                        cols = slice((block * 2 + half) * width, (block * 2 + half + 1) * width)
                        prompt_out[:, cols] = got[src, 2 * k + half, :pn, :]
                        answer_out[:, cols] = got[src, 2 * k + half, pn:, :]


def placed(zh, got, pn):
    rows, cols = got.shape[2], 16 * got.shape[3]
    vmem = pl.BlockSpec(memory_space=pltpu.VMEM)
    return pl.pallas_call(
        set_columns, out_shape=(jax.ShapeDtypeStruct((pn, cols), jnp.bfloat16), jax.ShapeDtypeStruct((rows - pn, cols), jnp.bfloat16)),
        in_specs=[pl.BlockSpec(memory_space=pltpu.SMEM), vmem], out_specs=(vmem, vmem),
        compiler_params=pltpu.CompilerParams(vmem_limit_bytes=16 * 2**20), name="set_columns",
    )(zh.reshape(1), got)


SEQ = ("x", "y", "zp", "zq")
HEAD = ("zh", "core")


def whole(pq, pk, pv, rq, rk, rv, lengths, table):
    side = lax.axis_index("zq").astype(jnp.int32)
    place = [lax.axis_index(n).astype(jnp.int32) for n in SEQ]
    mates = lax.dynamic_slice_in_dim(table, (place[0] * 4 + place[1]) * 4 + place[2] * 2, 2, 0)
    ends = jnp.cumsum(lengths)
    begun = jnp.where(mates[:, None] >= ends[None, :], ends[None, :], 0)
    zh = lax.axis_index("zh").astype(jnp.int32)
    place = jnp.concatenate([jnp.stack(place), mates, jnp.max(begun, axis=1), zh.reshape(1)])
    here, there = sorted_by_side(sort_keys, side, (pk, pv, rk, rv), 2 * D)
    keep, give = sorted_by_side(sort_queries, side, (pq, rq), rq.shape[1] // 2)
    swap = [(0, 1), (1, 0)]
    next_to = lax.ppermute(there, "zq", swap)
    far_same = lax.ppermute(here, "zp", swap)
    far_other = lax.ppermute(there, ("zp", "zq"), [(i, 3 - i) for i in range(4)])

    far_other, give = lax.optimization_barrier((far_other, give))
    got = lax.ppermute(give, "zq", swap)

    def ring(t, axis):
        up, down = [(i, (i + 1) % 4) for i in range(4)], [(i, (i - 1) % 4) for i in range(4)]
        before, after = lax.ppermute(t, axis, up), lax.ppermute(t, axis, down)
        n = t.shape[0] // 2
        return t, before, after, lax.ppermute(before[:n], axis, up), lax.ppermute(after[n:], axis, down)

    def colour(t, first, second):
        own, before, after, half_a, half_b = ring(t, first)
        return ring(jnp.stack([own, after, jnp.concatenate([half_a, half_b], axis=0), before]), second)

    gathered = (colour(jnp.stack([here, next_to]), "x", "y"), colour(jnp.stack([far_same, far_other]), "y", "x"))
    parts = lax.axis_size(HEAD)
    halves = attend(place, table, keep, got, gathered, parts)
    cross = [(i, 3 - i) for i in range(4)]
    moved = [lax.ppermute(h[1], ("zq", "zh"), cross) for h in halves]
    rest = jnp.stack([halves[0][0], halves[1][0], *moved], axis=1)
    back = lax.all_to_all(rest, ("core", "zq"), split_axis=0, concat_axis=0, tiled=True)
    return placed(zh, back, PR // parts)


def solution(mesh):
    grid = Mesh(mesh.devices.reshape(4, 4, 2, 2, 2, 2), SEQ + HEAD)
    both = P(SEQ, HEAD)
    rows = P(SEQ + HEAD, None)
    return jax.shard_map(whole, mesh=grid, in_specs=(both,) * 6 + (P(), P()), out_specs=(rows, rows), check_vma=False)
```

```python
import functools

import jax
import jax.numpy as jnp
from jax import lax
from jax.experimental import pallas as pl
from jax.experimental.pallas import tpu as pltpu
from jax.sharding import Mesh, PartitionSpec as P


D = 128
RB = 192
PR = 32
G = 8
CH = 512
LIMIT = 36 * 2**20
PER_EXP = 128 ** -0.5 * 1.4426950408889634
NEG = -1e30
RING = (((0, 0, 4),), ((3, 0, 4), (1, 0, 4)), ((2, 0, 4),))


def homes_of(groups):
    return [(colour, *h) for g in groups for colour in range(2) for h in RING[g]]


def kernel(place_ref, tab_ref, own_ref, got_ref, *refs, groups, last, region, mh, half):
    first = 0 in groups
    homes = homes_of(groups)
    pieces, refs = refs[:len(homes)], refs[len(homes):]
    if not first:
        before, refs = refs[:4], refs[4:]
    if last:
        outs, refs = refs[:2], refs[2:]
    m, a, pm, pa, kv, flags, qs, pqs, s0, s1, p0, p1, f0, f1 = refs
    px, py, pp, side = [place_ref[i] for i in range(4)]
    turn = 1 - 2 * place_ref[9]
    pair = (px * 4 + py) * 2 + pp
    prompts = sum(2 * n * PR for _, _, _, n in homes)
    nh, h0 = (G, 0) if half is None else (G // 2, half * (G // 2))
    per = nh // mh

    spans = [(place_ref[4 + t], place_ref[6 + t]) for t in range(2)]
    flags[:CH] = jnp.ones((CH, D), jnp.bfloat16)
    flags[CH:] = jnp.zeros((CH, D), jnp.bfloat16)

    def block(piece, r, t, i):
        kv[pl.ds(pl.multiple_of(t * region + prompts + i * RB, 64), RB), :] = piece[r, PR:, :]

    counts = (jnp.int32(0), jnp.int32(0))
    at = 0
    for piece, (colour, far, lead, n) in zip(pieces, homes):
        def bring(i, counts, piece=piece, colour=colour, far=far, lead=lead, at=at):
            near, e = i >> 1, i & 1
            dx, dy = (lead + near, far) if colour == 0 else (far, lead + near)
            slot = ((((px + turn * dx) & 3) * 4 + ((py + turn * dy) & 3)) * 2 + (pp ^ colour)) * 2 + (side ^ e)
            g = tab_ref[slot]
            new = []
            for t in range(2):
                kv[pl.ds(pl.multiple_of(t * region + (at + i) * PR, PR), PR), :] = piece[i, :PR, :]
                own, start = spans[t]
                hit = (g >= start) & (g < own)

                @pl.when(hit)
                def fetch(t=t):
                    block(piece, i, t, counts[t])

                new.append(counts[t] + hit.astype(jnp.int32))
            return tuple(new)

        counts = lax.fori_loop(0, 2 * n, bring, counts)
        at += 2 * n
    if first:
        for t in range(2):
            block(pieces[0], side ^ t, t, counts[t])
        counts = tuple(c + 1 for c in counts)
    keys = [prompts + c * RB for c in counts]
    chunks = [(k + CH - 1) // CH for k in keys]

    for src, t in ((own_ref, side), (got_ref, 1 - side)):
        for h in range(nh):
            cols = slice((h0 + h) * D, (h0 + h + 1) * D)
            qs[t * per + h // mh, pl.ds(h % mh * RB, RB)] = src[PR:, cols]
            pqs[pl.ds((t * nh + h) * PR, PR)] = src[:PR, cols]
    if first:
        for r in (m, pm):
            r[...] = jnp.full(r.shape, NEG, jnp.float32)
        for r in (a, pa):
            r[...] = jnp.zeros(r.shape, jnp.float32)
    elif half is None:
        for r, b in zip((m, a, pm, pa), before):
            r[...] = b[...]
    else:
        for t in range(2):
            for q in range(per):
                i, j = t * per + q, (2 * t + half) * per + q
                m[i], a[i] = before[0][j], before[1][j]
            pm[t], pa[t] = [b[t, half * nh * PR:(half + 1) * nh * PR] for b in before[2:]]
    for t in range(2):
        def pad(i, c, t=t):
            rows = pl.ds(pl.multiple_of(t * region + i * 64, 64), 64)
            kv[rows, :D] = kv[pl.ds(t * region, 64), :D]
            kv[rows, D:] = jnp.zeros((64, D), jnp.bfloat16)
            return c

        lax.fori_loop(keys[t] // 64, chunks[t] * (CH // 64), pad, 0)

    def soft(s, m_ref, i):
        old = m_ref[i]
        new = jnp.maximum(old, jnp.max(s, axis=1, keepdims=True))
        m_ref[i] = new
        spread = jnp.concatenate([new] * (s.shape[1] // D), axis=1)
        return jnp.exp2((s - spread) * PER_EXP).astype(jnp.bfloat16), jnp.exp2((old - new) * PER_EXP)

    def scores(q, start, n):
        return lax.dot_general(q, kv[pl.ds(start, n), :D], (((1,), (1,)), ((), ())), preferred_element_type=jnp.float32)

    def mixed(p, start, n, flag):
        v = jnp.concatenate([kv[pl.ds(start, n), D:], flag], axis=1)
        return lax.dot_general(p, v, (((1,), (0,)), ((), ())), preferred_element_type=jnp.float32)

    def both(f):
        return jnp.concatenate([f, f], axis=1)

    where = []
    for colour, far, lead, n in homes:
        lane = lax.broadcasted_iota(jnp.int32, (1, 2 * n * PR), 1)
        near, e = lead + (lane >> 6), (lane >> 5) & 1
        dx, dy = (near, jnp.int32(far)) if colour == 0 else (jnp.int32(far), near)
        slot = ((((px + turn * dx) & 3) * 4 + ((py + turn * dy) & 3)) * 2 + (pp ^ colour)) * 2 + (side ^ e)
        where.append(slot * PR + (lane & (PR - 1)))
    where = jnp.concatenate(where, axis=1)
    asked = nh * PR
    for t in range(2):
        row = (lax.broadcasted_iota(jnp.int32, (asked, 1), 0) & (PR - 1)) + (2 * pair + t) * PR
        s = jnp.where(where <= row, scores(pqs[t * asked:(t + 1) * asked], 0, prompts), NEG)
        p, factor = soft(s, pm, t)
        pa[t] = pa[t] * both(factor) + mixed(p, 0, prompts, jnp.ones((prompts, D), jnp.bfloat16))

    split, total = chunks[0] * per, (chunks[0] + chunks[1]) * per
    shift = per.bit_length() - 1

    def unit(u):
        t = (u >= split).astype(jnp.int32)
        v = u - t * split
        c, h = v >> shift, v & (per - 1)
        return t, c, t * per + h, pl.multiple_of(t * region + c * CH, CH)

    def stage_a(u, s):
        _, _, i, start = unit(u)
        s[...] = scores(qs[i], start, CH)

    def stage_b(u, s, p, f):
        t, c, i, _ = unit(u)
        x = s[...]
        if first:
            key = lax.broadcasted_iota(jnp.int32, (mh * RB, CH), 1)
            row = lax.broadcasted_iota(jnp.int32, (mh * RB, 1), 0)
            row = row % RB + (jnp.where(t == 0, keys[0], keys[1]) - RB - c * CH)
            x = jnp.where(key <= row, x, NEG)
        p[...], f[...] = soft(x, m, i)

    def stage_c(u, p, f):
        t, c, i, start = unit(u)
        live = jnp.minimum(jnp.where(t == 0, keys[0], keys[1]) - c * CH, CH)
        flag = flags[pl.ds(pl.multiple_of(CH - live, 64), CH), :]
        a[i] = a[i] * both(f[...]) + mixed(p[...], start, CH, flag)

    stage_a(0, s0)
    p1[...] = jnp.zeros(p1.shape, p1.dtype)
    f1[...] = jnp.ones(f1.shape, f1.dtype)

    def two(i, c):
        u = 2 * i
        stage_a(u + 1, s1)
        stage_b(u, s0, p0, f0)
        stage_c(jnp.maximum(u - 1, 0), p1, f1)
        stage_a(jnp.minimum(u + 2, total - 1), s0)
        stage_b(u + 1, s1, p1, f1)
        stage_c(u, p0, f0)
        return c

    lax.fori_loop(0, total >> 1, two, 0)
    stage_c(total - 1, p1, f1)

    if last:
        zh, n = place_ref[8], 2 * outs[0].shape[0] // 2
        pn, rn = PR // n, RB // n
        for t in range(2):
            for h in range(nh):
                cols = slice(h * D, (h + 1) * D)
                i, top = t * per + h // mh, h % mh * RB
                for k, out in enumerate(outs):
                    for core in range(2):
                        d = 2 * (zh ^ k) + core
                        rr = pl.ds(pl.multiple_of(h * PR + d * pn, 8), pn)
                        out[2 * core + t, :pn, cols] = (pa[t, rr, :D] / pa[t, rr, D:]).astype(jnp.bfloat16)
                        rr = pl.ds(pl.multiple_of(top + d * rn, 8), rn)
                        out[2 * core + t, pn:, cols] = (a[i, rr, :D] / a[i, rr, D:]).astype(jnp.bfloat16)


def attention(place, table, own, got, pieces, state, groups, parts, mh, half=None):
    slots = table.shape[0]
    f32, bf16 = jnp.float32, jnp.bfloat16
    smem = pl.BlockSpec(memory_space=pltpu.SMEM)
    vmem = pl.BlockSpec(memory_space=pltpu.VMEM)
    last = 2 in groups
    count = sum(2 * n for *_, n in homes_of(groups))
    region = -(-(count * PR + min(count, slots // 2) * RB) // CH) * CH

    def shapes_of(nh):
        units = 2 * nh // mh
        return [(units, mh * RB, D), (units, mh * RB, 2 * D), (2, nh * PR, D), (2, nh * PR, 2 * D)]

    nh = G if half is None else G // 2
    shapes, units = shapes_of(nh), 2 * nh // mh
    state = [x.reshape(shape) for x, shape in zip(state, shapes_of(G))]
    inputs = [place, table, own, got, *pieces, *state]
    kept = [jax.ShapeDtypeStruct(s, f32) for s in shapes]
    if last:
        out_shape, out_specs = (jax.ShapeDtypeStruct((parts, (PR + RB) // parts, nh * D), bf16),) * 2, (vmem, vmem)
    else:
        out_shape, out_specs = kept, [vmem] * 4
    flops = 4 * RB * nh * 2 * D * (count * (PR + RB // 2))
    return pl.pallas_call(
        functools.partial(kernel, groups=groups, last=last, region=region, mh=mh, half=half),
        out_shape=out_shape,
        in_specs=[smem, smem] + [vmem] * (len(inputs) - 2),
        out_specs=out_specs,
        scratch_shapes=([pltpu.VMEM(s, f32) for s in shapes] if last else []) + [
            pltpu.VMEM((2 * region, 2 * D), bf16),
            pltpu.VMEM((2 * CH, D), bf16),
            pltpu.VMEM((units, mh * RB, D), bf16),
            pltpu.VMEM((2 * nh * PR, D), bf16),
            pltpu.VMEM((mh * RB, CH), f32), pltpu.VMEM((mh * RB, CH), f32),
            pltpu.VMEM((mh * RB, CH), bf16), pltpu.VMEM((mh * RB, CH), bf16),
            pltpu.VMEM((mh * RB, D), f32), pltpu.VMEM((mh * RB, D), f32),
        ],
        cost_estimate=pl.CostEstimate(flops=flops, transcendentals=flops // 512, bytes_accessed=2**23),
        compiler_params=pltpu.CompilerParams(vmem_limit_bytes=LIMIT),
        name="attention",
    )(*inputs)


def attend(place, table, own, got, gathered, parts):
    gathered = [[p.reshape(-1, *p.shape[2:]) for p in c] for c in gathered]
    run = functools.partial(attention, place, table, own, got)
    state = run([c[0] for c in gathered], (), (0,), parts, 2)
    state = run([p for c in gathered for p in c[1:3]], state, (1,), parts, 4)
    return [run([p for c in gathered for p in c[3:]], state, (2,), parts, 2, half) for half in range(2)]


def together(copies):
    for c in copies:
        c.start()
    for c in copies:
        c.wait()


def sort_keys(side_ref, pk, pv, rk, rv, here, there, sems):
    side = side_ref[0]
    copies = []
    for out, j in ((here, side), (there, 1 - side)):
        for rows, k, v in ((pl.ds(0, PR), pk, pv), (pl.ds(PR, RB), rk, rv)):
            for w, src in enumerate((k, v)):
                copies.append(pltpu.make_async_copy(
                    src.at[:, pl.ds(pl.multiple_of(j * D, D), D)], out.at[rows, pl.ds(w * D, D)], sems.at[len(copies)]))
    together(copies)


def sort_queries(side_ref, pq, rq, keep, give, sems):
    side, half = side_ref[0], keep.shape[1]
    copies = []
    for out, j in ((keep, side), (give, 1 - side)):
        for rows, src in ((pl.ds(0, PR), pq), (pl.ds(PR, RB), rq)):
            copies.append(pltpu.make_async_copy(
                src.at[:, pl.ds(pl.multiple_of(j * half, half), half)], out.at[rows], sems.at[len(copies)]))
    together(copies)


def sorted_by_side(body, side, arrays, cols):
    out = jax.ShapeDtypeStruct((PR + RB, cols), jnp.bfloat16)
    vmem = pl.BlockSpec(memory_space=pltpu.VMEM)
    return pl.pallas_call(
        body, out_shape=(out, out),
        in_specs=[pl.BlockSpec(memory_space=pltpu.SMEM)] + [pl.BlockSpec(memory_space=pltpu.HBM)] * len(arrays),
        out_specs=(vmem, vmem), scratch_shapes=[pltpu.SemaphoreType.DMA((2 * len(arrays),))],
        compiler_params=pltpu.CompilerParams(vmem_limit_bytes=8 * 2**20),
    )(side.reshape(1), *arrays)


def set_columns(zh_ref, got, prompt_out, answer_out):
    pn, width = prompt_out.shape[0], got.shape[3]
    for zh in range(2):
        @pl.when(zh_ref[0] == zh)
        def write(zh=zh):
            for src in range(4):
                core, zq = src >> 1, src & 1
                for k in range(2):
                    block = ((zh ^ k) * 2 + core) * 2 + (zq ^ k)
                    for half in range(2):
                        cols = slice((block * 2 + half) * width, (block * 2 + half + 1) * width)
                        prompt_out[:, cols] = got[src, 2 * k + half, :pn, :]
                        answer_out[:, cols] = got[src, 2 * k + half, pn:, :]


def placed(zh, got, pn):
    rows, cols = got.shape[2], 16 * got.shape[3]
    vmem = pl.BlockSpec(memory_space=pltpu.VMEM)
    return pl.pallas_call(
        set_columns, out_shape=(jax.ShapeDtypeStruct((pn, cols), jnp.bfloat16), jax.ShapeDtypeStruct((rows - pn, cols), jnp.bfloat16)),
        in_specs=[pl.BlockSpec(memory_space=pltpu.SMEM), vmem], out_specs=(vmem, vmem),
        compiler_params=pltpu.CompilerParams(vmem_limit_bytes=16 * 2**20), name="set_columns",
    )(zh.reshape(1), got)


SEQ = ("x", "y", "zp", "zq")
HEAD = ("zh", "core")


def whole(pq, pk, pv, rq, rk, rv, lengths, table):
    side = lax.axis_index("zq").astype(jnp.int32)
    place = [lax.axis_index(n).astype(jnp.int32) for n in SEQ]
    mates = lax.dynamic_slice_in_dim(table, (place[0] * 4 + place[1]) * 4 + place[2] * 2, 2, 0)
    ends = jnp.cumsum(lengths)
    begun = jnp.where(mates[:, None] >= ends[None, :], ends[None, :], 0)
    zh = lax.axis_index("zh").astype(jnp.int32)
    place = jnp.concatenate([jnp.stack(place), mates, jnp.max(begun, axis=1), zh.reshape(1),
                             lax.axis_index("core").astype(jnp.int32).reshape(1)])
    here, there = sorted_by_side(sort_keys, side, (pk, pv, rk, rv), 2 * D)
    keep, give = sorted_by_side(sort_queries, side, (pq, rq), rq.shape[1] // 2)
    swap = [(0, 1), (1, 0)]
    next_to = lax.ppermute(there, "zq", swap)
    far_same = lax.ppermute(here, "zp", swap)
    far_other = lax.ppermute(there, ("zp", "zq"), [(i, 3 - i) for i in range(4)])

    far_other, give = lax.optimization_barrier((far_other, give))
    got = lax.ppermute(give, "zq", swap)

    def ring(t, axis):
        ahead = [(2 * i + c, (i + 1 - 2 * c) % 4 * 2 + c) for i in range(4) for c in range(2)]
        astern = [(b, a) for a, b in ahead]
        first = lax.ppermute(t, (axis, "core"), ahead)
        second = lax.ppermute(t, (axis, "core"), astern)
        return t, first, second, lax.ppermute(first, (axis, "core"), ahead)

    def colour(t, first, second):
        own, before, after, far = ring(t, first)
        return ring(jnp.stack([own, after, far, before]), second)

    gathered = (colour(jnp.stack([here, next_to]), "x", "y"), colour(jnp.stack([far_same, far_other]), "y", "x"))
    parts = lax.axis_size(HEAD)
    halves = attend(place, table, keep, got, gathered, parts)
    cross = [(i, 3 - i) for i in range(4)]
    moved = [lax.ppermute(h[1], ("zq", "zh"), cross) for h in halves]
    rest = jnp.stack([halves[0][0], halves[1][0], *moved], axis=1)
    back = lax.all_to_all(rest, ("core", "zq"), split_axis=0, concat_axis=0, tiled=True)
    return placed(zh, back, PR // parts)


def solution(mesh):
    grid = Mesh(mesh.devices.reshape(4, 4, 2, 2, 2, 2), SEQ + HEAD)
    both = P(SEQ, HEAD)
    rows = P(SEQ + HEAD, None)
    return jax.shard_map(whole, mesh=grid, in_specs=(both,) * 6 + (P(), P()), out_specs=(rows, rows), check_vma=False)
```
